8 devices in a mesh: batch: 1 (over z), row: 2 (over y), col: 4 (over x, core).
Axes of the slice: x: 2, y: 2, z: 1, core: 2. Of those that a mesh axis runs over, the one named last changes fastest.
Arguments:
- lower_tri: bfloat16 [2048, 2048], P(('batch', 'row'), 'col')
- right_side: bfloat16 [2048, 16384], P(('batch', 'row'), 'col')
- grad_out: bfloat16 [2048, 16384], P(('batch', 'row'), 'col')
Outputs:
- output 1: bfloat16 [2048, 16384], P(('batch', 'row'), 'col')
- output 2: bfloat16 [2048, 2048], P(('batch', 'row'), 'col')
All inputs are finite; a program needn't handle non-finite values.
Results may differ from the reference program's by a relative error of at most 0.001.
Values are sent between devices in bfloat16 or wider.
A program may use at most 1 GiB of HBM per device.

```python
import jax
import jax.numpy as jnp

MAT_ORDER = 2048
BLOCK_SIZE = 256
RHS_COLS = 16384
MESH_ROWS = 2
MESH_COLS = 4
ROW_BLOCKS = MAT_ORDER // (BLOCK_SIZE * MESH_ROWS)
COL_BLOCKS = MAT_ORDER // (BLOCK_SIZE * MESH_COLS)


def rows_to_global(stored):
    num_cols = stored.shape[1]
    return stored.reshape(MESH_ROWS, ROW_BLOCKS, BLOCK_SIZE, num_cols).transpose(1, 0, 2, 3).reshape(MAT_ORDER, num_cols)


def rows_to_stored(natural):
    num_cols = natural.shape[1]
    return natural.reshape(ROW_BLOCKS, MESH_ROWS, BLOCK_SIZE, num_cols).transpose(1, 0, 2, 3).reshape(MAT_ORDER, num_cols)


def cols_to_global(stored):
    num_rows = stored.shape[0]
    return stored.reshape(num_rows, MESH_COLS, COL_BLOCKS, BLOCK_SIZE).transpose(0, 2, 1, 3).reshape(num_rows, MAT_ORDER)


def cols_to_stored(natural):
    num_rows = natural.shape[0]
    return natural.reshape(num_rows, COL_BLOCKS, MESH_COLS, BLOCK_SIZE).transpose(0, 2, 1, 3).reshape(num_rows, MAT_ORDER)


def setup_inputs(seed: int = 0, part: int = 0) -> dict:
    base_key = jax.random.fold_in(jax.random.key(seed), part)
    key_lower, key_right, key_grad = jax.random.split(base_key, 3)
    lower_mat = jax.random.normal(key_lower, (MAT_ORDER, MAT_ORDER), jnp.float32) * (MAT_ORDER ** -0.5)
    lower_mat = jnp.tril(lower_mat).astype(jnp.bfloat16)
    right_mat = jax.random.normal(key_right, (MAT_ORDER, RHS_COLS), jnp.float32) * (RHS_COLS ** -0.5)
    grad_mat = jax.random.normal(key_grad, (MAT_ORDER, RHS_COLS), jnp.float32)
    return {
        "lower_tri": cols_to_stored(rows_to_stored(lower_mat)),
        "right_side": rows_to_stored(right_mat.astype(jnp.bfloat16)),
        "grad_out": rows_to_stored(grad_mat.astype(jnp.bfloat16)),
    }


def reference(lower_tri, right_side, grad_out):
    lower_mat = cols_to_global(rows_to_global(lower_tri))
    right_mat = rows_to_global(right_side)
    grad_mat = rows_to_global(grad_out)
    grad_right = jnp.dot(lower_mat.T, grad_mat, preferred_element_type=jnp.float32)
    grad_lower = jnp.tril(jnp.dot(grad_mat, right_mat.T, preferred_element_type=jnp.float32))
    return (rows_to_stored(grad_right.astype(jnp.bfloat16)), cols_to_stored(rows_to_stored(grad_lower.astype(jnp.bfloat16))))
```

```python
import functools

import jax
import jax.numpy as jnp
from jax import lax
from jax.experimental import pallas as pl
from jax.experimental.pallas import tpu as pltpu
from jax.sharding import PartitionSpec as P

BLK = 256
AXES = ("row", "col")
F32 = jnp.float32
BF16 = jnp.bfloat16


def dev(r, x, core):
    return r * 4 + x * 2 + core


ALL = [(r, x, core) for r in range(2) for x in range(2) for core in range(2)]
FLIP_ROW = [(dev(r, x, c), dev(1 - r, x, c)) for r, x, c in ALL]


def send(value, pairs):
    return lax.ppermute(value, AXES, pairs)


def rows_kernel(num_terms, *refs):
    weights, blocks, out = refs[:num_terms], refs[num_terms:2 * num_terms], refs[-1]
    total = None
    for weight, block in zip(weights, blocks):
        part = lax.dot_general(weight[...], block[...], (((0,), (0,)), ((), ())), preferred_element_type=F32)
        total = part if total is None else total + part
    out[...] = total.astype(out.dtype)


def tail_kernel(acc, weight, block, old, out):
    part = lax.dot_general(weight[...], block[...], (((0,), (0,)), ((), ())), preferred_element_type=F32)
    out[...] = (acc[...] + part).astype(out.dtype)


def block_row(weights, local, local_ids, remote, out_row, out_shape, out_dtype, old=None, tile=1024):
    num_cols = local.shape[1]
    num_terms = len(weights)
    specs = [pl.BlockSpec((BLK, BLK), lambda j: (0, 0)) for _ in weights]
    specs += [pl.BlockSpec((BLK, tile), functools.partial(lambda p, j: (p, j), p)) for p in local_ids]
    specs += [pl.BlockSpec((BLK, tile), lambda j: (0, j)) for _ in remote]
    args = list(weights) + [local] * len(local_ids) + list(remote)
    aliases = {}
    if old is not None:
        specs.append(pl.BlockSpec(memory_space=pl.ANY))
        aliases = {len(args): 0}
        args.append(old)
    return pl.pallas_call(
        functools.partial(rows_kernel, num_terms),
        grid=(num_cols // tile,),
        in_specs=specs,
        out_specs=pl.BlockSpec((BLK, tile), lambda j: (out_row, j)),
        out_shape=jax.ShapeDtypeStruct(out_shape, out_dtype),
        input_output_aliases=aliases,
        cost_estimate=pl.CostEstimate(flops=2 * num_terms * BLK * BLK * num_cols, bytes_accessed=2 * num_terms * BLK * num_cols, transcendentals=0),
    )(*args)


def add_tail(acc, weight, block, old, first_tile, tile):
    cols = block.shape[1]
    return pl.pallas_call(
        tail_kernel,
        grid=(cols // tile,),
        in_specs=[
            pl.BlockSpec((BLK, tile), lambda j: (0, first_tile + j)),
            pl.BlockSpec((BLK, BLK), lambda j: (0, 0)),
            pl.BlockSpec((BLK, tile), lambda j: (0, j)),
            pl.BlockSpec(memory_space=pl.ANY),
        ],
        out_specs=pl.BlockSpec((BLK, tile), lambda j: (0, first_tile + j)),
        out_shape=jax.ShapeDtypeStruct(old.shape, old.dtype),
        input_output_aliases={3: 0},
        cost_estimate=pl.CostEstimate(flops=2 * BLK * BLK * cols, bytes_accessed=8 * BLK * cols, transcendentals=0),
    )(acc, weight, block, old)


def after(value, *others):
    return lax.optimization_barrier((value, *others))[0]


def outer(left, right):
    return lax.dot_general(left, right, (((1,), (1,)), ((), ())), preferred_element_type=F32)


def per_device(lower, side, grad):
    r = lax.axis_index("row")
    col = lax.axis_index("col")
    x, core = col // 2, col % 2
    x0 = x == 0
    num_cols = grad.shape[1]
    split = num_cols - 1024

    near = jnp.concatenate([lower[BLK:, :BLK], lower[3 * BLK:, BLK:]], axis=0)
    far = jnp.concatenate([lower[:BLK, :BLK], lower[2 * BLK:3 * BLK, BLK:]], axis=0)
    near_in = send(near, [(dev(1 - q, xx, q), dev(q, xx, q)) for q in range(2) for xx in range(2)])

    got = {}
    for p in (3, 2, 1):
        got[p] = send(grad[p * BLK:(p + 1) * BLK], FLIP_ROW)
    first = jnp.where(r == 1, grad[:BLK], side[:BLK])
    got_first = [send(first[:, :split], FLIP_ROW), send(first[:, split:], FLIP_ROW)]

    local_x = send(lower, [(dev(q, xx, q), dev(q, 1 - xx, q)) for q in range(2) for xx in range(2)])
    far_side = send(far, [(dev(1, 0, 0), dev(1, 1, 0))])
    far_in = send(far_side, [(dev(1, 1, 0), dev(0, 1, 0))])
    swap = send(jnp.concatenate([near_in, far_in], axis=0), [(dev(q, xx, q), dev(q, 1 - xx, q)) for q in range(2) for xx in range(2)])
    near0 = jnp.where(x0, near_in, swap[:4 * BLK])
    near1 = jnp.where(x0, swap[:4 * BLK], near_in)
    far0 = jnp.where(x0, swap[4 * BLK:], far_in)
    local0 = jnp.where(x0, lower, local_x)
    local1 = jnp.where(x0, local_x, lower)
    pack = jnp.concatenate([near0, near1, far0, local0[:, :BLK], local1[:, :BLK], local0[2 * BLK:, BLK:], local1[2 * BLK:, BLK:]], axis=0)
    pack_in = send(pack, [(dev(q, xx, q), dev(q, xx, 1 - q)) for q in range(2) for xx in range(2)])
    pack = jnp.where(core == r, pack, pack_in)

    def cut(i):
        return pack[i * BLK:(i + 1) * BLK]

    far_w = {(1, 0): 0, (2, 0): 1, (3, 0): 2, (3, 2): 3, (1, 1): 4, (2, 1): 5, (3, 1): 6, (3, 3): 7, (0, 0): 8, (2, 2): 9}
    far_w = {pq: cut(i) for pq, i in far_w.items()}
    near_w = {}
    for p in range(4):
        near_w[p, 0] = cut(10 + p)
        near_w[p, 1] = cut(14 + p)
    for p in (2, 3):
        near_w[p, 2] = cut(18 + p - 2)
        near_w[p, 3] = cut(20 + p - 2)

    own_push = [(dev(q, xx, 1 - q), dev(q, xx, q)) for q in range(2) for xx in range(2)]
    own_cross = [(dev(q, xx, q), dev(q, 1 - xx, q)) for q in range(2) for xx in range(2)]

    def halves(total):
        blocks = [total[:, i * BLK:(i + 1) * BLK] for i in range(total.shape[1] // BLK)]
        if len(blocks) == 3:
            blocks.append(jnp.zeros_like(blocks[0]))
        evens = jnp.concatenate(blocks[0::2], axis=1)
        odds = jnp.concatenate(blocks[1::2], axis=1)
        return jnp.where(x0, evens, odds), jnp.where(x0, odds, evens)

    def padded(part):
        return jnp.pad(part, ((0, 0), (0, 4 * BLK - part.shape[1])))

    local_part = jnp.concatenate([padded(outer(grad[p * BLK:(p + 1) * BLK], side[:(p + 1) * BLK])) for p in range(4)], axis=0)
    local_pushed = send(local_part, own_push)

    shape = grad.shape
    pairs = [(dev(rr, xx, rr), dev(1 - rr, xx, rr)) for rr in range(2) for xx in range(2)]
    back = {}

    def row_of_blocks(q, out):
        ids = list(range(q, 4))
        return block_row([near_w[p, q] for p in ids] + [far_w[p, q] for p in ids], grad, ids, [got[p] for p in ids], q, shape, BF16, out)

    got[3] = after(got[3], pack, local_part)
    part3 = outer(got[3], side)
    pushed3 = send(part3, own_push)
    out = row_of_blocks(3, None)
    mine_local, theirs_local = halves(local_part + local_pushed)
    mine3, theirs3 = halves(part3 + pushed3)
    crossed3 = send(theirs3, own_cross)
    crossed_local = send(theirs_local, own_cross)

    got[2] = after(got[2], out, theirs3, theirs_local)
    part2 = outer(got[2], side[:3 * BLK])
    pushed2 = send(part2, own_push)
    out = row_of_blocks(2, out)
    mine2, theirs2 = halves(part2 + pushed2)
    crossed2 = send(theirs2, own_cross)
    local_sum = (mine_local + crossed_local).astype(BF16)
    sum3 = (mine3 + crossed3).astype(BF16)
    back[3] = send(sum3, pairs)

    got[1] = after(got[1], out, theirs2, sum3, local_sum)
    part1 = outer(got[1], side[:2 * BLK])
    pushed1 = send(part1, own_push)
    out = row_of_blocks(1, out)
    acc = block_row([near_w[p, 0] for p in range(4)] + [far_w[p, 0] for p in (1, 2, 3)], grad, [0, 1, 2, 3], [got[p] for p in (1, 2, 3)], 0, (BLK, num_cols), F32)
    mine1, theirs1 = halves(part1 + pushed1)
    crossed1 = send(theirs1, own_cross)
    sum2 = (mine2 + crossed2).astype(BF16)
    sum1 = (mine1 + crossed1).astype(BF16)
    half2 = send(sum2[:, :BLK], pairs)
    other2 = send(sum2[:, BLK:], [(dev(0, 0, 0), dev(1, 0, 0))])
    back[2] = jnp.concatenate([half2, other2], axis=1)
    half1 = send(sum1, [p for p in pairs if p[0] != dev(1, 1, 1)])
    back[1] = jnp.concatenate([half1, jnp.zeros_like(half1)], axis=1)

    got_first[0] = after(got_first[0], out, acc, sum1, sum2)
    corner0 = outer(grad[:BLK, :split], got_first[0])
    out = add_tail(acc, far_w[0, 0], got_first[0], out, 0, 1024)
    got_first[1] = after(got_first[1], out, corner0)
    corner = corner0 + outer(grad[:BLK, split:], got_first[1])
    corner_in = send(corner, [(dev(1, xx, 1), dev(1, xx, 0)) for xx in range(2)])
    out = add_tail(acc, far_w[0, 0], got_first[1], out, split // 1024, 1024)
    corner = corner + corner_in
    corner = corner + send(corner, [(dev(1, 1, 0), dev(1, 0, 0))])
    corner = jnp.where((r == 1) & (col == 0), corner, 0.0).astype(BF16)
    back0 = jnp.pad(corner, ((0, 0), (0, BLK)))
    far_sum = jnp.concatenate([back0, back[1], back[2], back[3]], axis=0)
    lower_out = jnp.where(core == r, local_sum, far_sum)
    row_pos = jnp.arange(lower.shape[0])[:, None]
    col_pos = jnp.arange(lower.shape[1])[None, :]
    row_global = (row_pos // BLK * 2 + r) * BLK + row_pos % BLK
    col_global = (col_pos // BLK * 4 + col) * BLK + col_pos % BLK
    lower_out = jnp.where(row_global >= col_global, lower_out, jnp.zeros((), BF16))
    return out, lower_out


def solution(mesh):
    spec = P(("batch", "row"), "col")
    return jax.shard_map(per_device, mesh=mesh, in_specs=(spec, spec, spec), out_specs=(spec, spec), check_vma=False)
```

```python
import jax
import jax.numpy as jnp
from jax import lax
from jax.experimental import pallas as pl
from jax.experimental.pallas import tpu as pltpu
from jax.sharding import PartitionSpec as P

BLK = 256
F32 = jnp.float32
BF16 = jnp.bfloat16
MESH = pl.DeviceIdType.MESH
TILE = 512
EARLY = ((0, 2048),)
LATE = ((2048, 1024), (3072, 512), (3584, 512))
CHUNKS = EARLY + LATE
LOCAL_SLOTS = ((0, 0), (1, 0), (2, 0), (3, 0), (2, 1), (3, 1))
FAR_SLOTS = ((3, 0), (3, 1), (2, 0), (2, 1), (1, 0))
NUM_LOCAL = len(LOCAL_SLOTS)
NUM_SLOTS = NUM_LOCAL + len(FAR_SLOTS)
GROUPS = ((0, 6), (6, 8), (8, 10), (10, 11))


def rows(p, n=1):
    return pl.ds(p * BLK, n * BLK)


def kernel(lower, side, grad, db, dl, xr, xl, bl, acc, wl, wr, part, peer, cross, done, corner,
           bulk_s, bulk_r, load_s, wl_s, wl_r, near_s, near_r, far_s, far_r, push_s, push_r, cross_s, cross_r, back_s, back_r, corner_s, corner_r):
    r = lax.axis_index("row")
    c = lax.axis_index("col")
    x = c // 2
    core = c % 2
    own = core == r
    other = core != r
    across = {"row": 1 - r}
    mate = {"col": 2 * x + 1 - core}
    next_chip = {"col": 2 * (1 - x) + core}
    diagonal = {"col": 2 * (1 - x) + 1 - core}
    num_cols = grad.shape[1]
    sent = []

    def copy_to(device, src, dst, send_sem, recv_sem):
        return pltpu.make_async_remote_copy(src_ref=src, dst_ref=dst, send_sem=send_sem, recv_sem=recv_sem, device_id=device, device_id_type=MESH)

    def start(when, copy):
        sent.append((when, copy))
        if when is None:
            copy.start()
        else:
            pl.when(when)(copy.start)

    def arrived(ref, sem):
        pltpu.make_async_copy(ref, ref, sem).wait()

    barrier = pltpu.get_barrier_semaphore()
    for device in (across, mate, next_chip, diagonal):
        pl.semaphore_signal(barrier, inc=1, device_id=device, device_id_type=MESH)
    pl.semaphore_wait(barrier, 4)

    near_src = (lower.at[pl.ds(BLK, 3 * BLK), pl.ds(0, BLK)], lower.at[pl.ds(3 * BLK, BLK), pl.ds(BLK, BLK)])
    far_src = (lower.at[pl.ds(0, BLK), pl.ds(0, BLK)], lower.at[pl.ds(2 * BLK, BLK), pl.ds(BLK, BLK)])

    def near_dst(q, h):
        return wr.at[q, rows(1, 3)] if h == 0 else wr.at[q, rows(3)]

    def far_dst(q):
        return wr.at[q, rows(q)]

    for h in range(2):
        start(other, copy_to(across, near_src[h], near_dst(x + 2 * h, h), near_s.at[h], near_r.at[x + 2 * h]))
    far_sender = other & (r == 1) & (x == 0)
    for h in range(2):
        start(far_sender, copy_to(across, far_src[h], far_dst(2 * h), far_s.at[h], far_r.at[h]))

    def bulk(i, p):
        return copy_to(across, grad.at[rows(p)], xr.at[rows(p)], bulk_s.at[i], bulk_r.at[i])

    start(None, bulk(0, 3))
    start(None, bulk(1, 2))

    loads = [pltpu.make_async_copy(side.at[rows(q)], bl.at[rows(q)], load_s.at[q]) for q in range(4)]
    loads += [pltpu.make_async_copy(grad.at[rows(p)], xl.at[rows(p)], load_s.at[4 + p]) for p in range(4)]
    for load in loads:
        load.start()

    for h in range(2):
        src = lower.at[:, pl.ds(0, BLK)] if h == 0 else lower.at[rows(2, 2), pl.ds(BLK, BLK)]
        q = x + 2 * h
        dst = wl.at[q] if h == 0 else wl.at[q, rows(2, 2)]
        pl.when(own)(pltpu.make_async_copy(src, dst, wl_r.at[q]).start)
        for n, device in enumerate((mate, next_chip, diagonal)):
            start(own, copy_to(device, src, dst, wl_s.at[3 * h + n], wl_r.at[q]))

    @pl.when(r == 1)
    def _():
        wr[2, rows(2)] = jnp.zeros((BLK, BLK), BF16)

    for p in range(4):
        for h in range(2):
            far_zero = (x + 2 * h > p + r - 1) if p else (x >= 0)
            zero = (other & far_zero) | (own & (x + 2 * h > p))

            @pl.when(zero)
            def _():
                dl[rows(p), rows(h)] = jnp.zeros((BLK, BLK), BF16)

    def outer(left, left_row, q):
        total = None
        for k in range(0, num_cols, 1024):
            term = lax.dot_general(left[pl.ds(left_row, BLK), pl.ds(k, 1024)], bl[pl.ds(q * BLK, BLK), pl.ds(k, 1024)], (((1,), (1,)), ((), ())), preferred_element_type=F32)
            total = term if total is None else total + term
        return total

    for load in loads:
        load.wait()

    def local_outer(i, carry):
        slot, parity = i // 2, i % 2
        h = slot // 4
        p = slot - 2 * h
        part[slot, parity] = outer(xl, pl.multiple_of(p * BLK, BLK), 2 * h + parity)
        return carry

    lax.fori_loop(0, 2 * NUM_LOCAL, local_outer, 0)

    for h in range(2):
        q = x + 2 * h

        @pl.when(own)
        def _():
            arrived(near_dst(q, h), near_r.at[q])

        for n, device in enumerate((mate, next_chip, diagonal)):
            start(own, copy_to(device, near_dst(q, h), near_dst(q, h), near_s.at[2 + 3 * h + n], near_r.at[q]))
    far_owner = own & (r == 0) & (x == 0)
    for h in range(2):

        @pl.when(far_owner)
        def _():
            arrived(far_dst(2 * h), far_r.at[h])

        for n, device in enumerate((mate, next_chip, diagonal)):
            start(far_owner, copy_to(device, far_dst(2 * h), far_dst(2 * h), far_s.at[2 + 3 * h + n], far_r.at[h]))

    def push(g):
        lo, hi = GROUPS[g]
        span = pl.ds(lo, hi - lo)
        start(other, copy_to(mate, part.at[span], peer.at[span], push_s.at[g], push_r.at[g]))

    def add_and_cross(g):
        lo, hi = GROUPS[g]
        span = pl.ds(lo, hi - lo)

        @pl.when(own)
        def _():
            arrived(peer.at[span], push_r.at[g])

            def add(slot, carry):
                part[slot] = part[slot] + peer[slot]
                return carry

            lax.fori_loop(lo, hi, add, 0)

        start(own, copy_to(next_chip, part.at[span, 1 - x], cross.at[span], cross_s.at[g], cross_r.at[g]))

    def wait_cross(g):
        lo, hi = GROUPS[g]
        arrived(cross.at[pl.ds(lo, hi - lo)], cross_r.at[g])

    def back_copies(i):
        p, h = FAR_SLOTS[i]
        return copy_to(across, done.at[i], dl.at[rows(p), rows(h)], back_s.at[i], back_r.at[i])

    def finish_far(g):
        lo, hi = GROUPS[g]

        @pl.when(own)
        def _():
            wait_cross(g)
            for slot in range(lo, hi):
                done[slot - NUM_LOCAL] = (part[slot, x] + cross[slot]).astype(BF16)

        for slot in range(lo, hi):
            p, h = FAR_SLOTS[slot - NUM_LOCAL]
            start(own & (x + 2 * h <= p - r), back_copies(slot - NUM_LOCAL))

    def finish_local():
        @pl.when(own)
        def _():
            wait_cross(0)
            below = lax.broadcasted_iota(jnp.int32, (BLK, BLK), 0) >= lax.broadcasted_iota(jnp.int32, (BLK, BLK), 1)
            for slot, (p, h) in enumerate(LOCAL_SLOTS):
                q = x + 2 * h

                @pl.when(q <= p)
                def _():
                    total = part[slot, x] + cross[slot]
                    keep = below | (q < p)
                    dl[rows(p), rows(h)] = jnp.where(keep, total, 0.0).astype(BF16)

    def far_outer(p, lo, num_q):
        def body(q, carry):
            part[lo + q // 2, q % 2] = outer(xr, p * BLK, q)
            return carry

        lax.fori_loop(0, num_q, body, 0)

    def row_sum(q, far_first, cols):
        near = lax.dot_general(wl[q, rows(q, 4 - q)], xl[rows(q, 4 - q), cols], (((0,), (0,)), ((), ())), preferred_element_type=F32)
        far = lax.dot_general(wr[q, rows(far_first, 4 - far_first)], xr[rows(far_first, 4 - far_first), cols], (((0,), (0,)), ((), ())), preferred_element_type=F32)
        return near + far

    def tile_loop(body):
        def step(j, carry):
            body(pl.ds(pl.multiple_of(j * TILE, TILE), TILE))
            return carry

        lax.fori_loop(0, num_cols // TILE, step, 0)

    def weights_here(q):
        h = q // 2
        arrived(wl.at[q] if h == 0 else wl.at[q, rows(2, 2)], wl_r.at[q])
        if h == 0:
            pl.when(other | (x != q))(lambda: arrived(near_dst(q, h), near_r.at[q]))
        else:
            pl.when(other | (x + 2 != q))(lambda: arrived(near_dst(q, h), near_r.at[q]))
        if q % 2 == 0:
            pl.when((r == 0) & jnp.logical_not(far_owner))(lambda: arrived(far_dst(q), far_r.at[h]))

    def block_row(q):
        weights_here(q)

        def body(cols):
            db[rows(q), cols] = row_sum(q, q, cols).astype(BF16)

        tile_loop(body)

    def chunk_copy(i):
        first, width = CHUNKS[i]
        cols = pl.ds(first, width)
        sems = bulk_s.at[3 + i], bulk_r.at[3 + i]
        dst = xr.at[rows(0), cols]
        return copy_to(across, grad.at[rows(0), cols], dst, *sems), copy_to(across, side.at[rows(0), cols], dst, *sems)

    def start_chunks(when, span):
        for i in span:
            from_grad, from_side = chunk_copy(i)
            start(when & (r == 1), from_grad)
            start(when & (r == 0), from_side)

    arrived(xr.at[rows(3)], bulk_r.at[0])
    push(0)
    far_outer(3, 6, 4)
    block_row(3)
    start(None, bulk(2, 1))
    push(1)
    add_and_cross(0)
    add_and_cross(1)

    arrived(xr.at[rows(2)], bulk_r.at[1])
    finish_far(1)
    early = range(len(EARLY))
    late = range(len(EARLY), len(CHUNKS))
    start_chunks(core >= 0, early)
    far_outer(2, 8, 4)
    block_row(2)
    push(2)
    finish_local()
    add_and_cross(2)

    arrived(xr.at[rows(1)], bulk_r.at[2])
    last_sender = own & (r == 1)
    start_chunks(jnp.logical_not(last_sender), late)
    finish_far(2)
    far_outer(1, 10, 2)
    block_row(1)
    push(3)
    weights_here(0)

    def first_row(cols):
        total = row_sum(0, 1, cols)

        @pl.when(r == 1)
        def _():
            db[rows(0), cols] = total.astype(BF16)

        @pl.when(r == 0)
        def _():
            acc[:, cols] = total

    def first_half(lo, hi):
        def step(j, carry):
            first_row(pl.ds(pl.multiple_of(j * TILE, TILE), TILE))
            return carry

        lax.fori_loop(lo, hi, step, 0)

    add_and_cross(3)
    first_half(0, num_cols // TILE)
    finish_far(3)
    start_chunks(last_sender, late)

    @pl.when(r == 1)
    def _():
        corner[0] = jnp.zeros((BLK, BLK), F32)

    for i, (first, width) in enumerate(CHUNKS):
        arrived(xr.at[rows(0), pl.ds(first, width)], bulk_r.at[3 + i])

        def step(j, carry):
            cols = pl.ds(pl.multiple_of(first + j * TILE, TILE), TILE)

            @pl.when(r == 0)
            def _():
                term = lax.dot_general(wr[0, rows(0)], xr[rows(0), cols], (((0,), (0,)), ((), ())), preferred_element_type=F32)
                db[rows(0), cols] = (acc[:, cols] + term).astype(BF16)

            @pl.when(r == 1)
            def _():
                corner[0] += lax.dot_general(xl[rows(0), cols], xr[rows(0), cols], (((1,), (1,)), ((), ())), preferred_element_type=F32)

            return carry

        lax.fori_loop(0, width // TILE, step, 0)

    corner_owner = (r == 1) & (core == 0)
    start((r == 1) & (core == 1), copy_to(mate, corner.at[0], corner.at[1], corner_s.at[0], corner_r.at[0]))

    @pl.when(corner_owner)
    def _():
        arrived(corner.at[1], corner_r.at[0])
        corner[0] += corner[1]

    start(corner_owner & (x == 1), copy_to(next_chip, corner.at[0], corner.at[2], corner_s.at[1], corner_r.at[1]))

    @pl.when(corner_owner & (x == 0))
    def _():
        arrived(corner.at[2], corner_r.at[1])
        dl[rows(0), rows(0)] = (corner[0] + corner[2]).astype(BF16)

    for i, (p, h) in enumerate(FAR_SLOTS):
        pl.when(other & (x + 2 * h <= p + r - 1))(lambda: arrived(dl.at[rows(p), rows(h)], back_r.at[i]))
    for when, copy in sent:
        if when is None:
            copy.wait_send()
        else:
            pl.when(when)(copy.wait_send)


def per_device(lower, side, grad):
    num_rows, num_cols = grad.shape
    dma = pltpu.SemaphoreType.DMA
    num_bulk = 3 + len(CHUNKS)
    return pl.pallas_call(
        kernel,
        in_specs=[pl.BlockSpec(memory_space=pl.ANY)] * 3,
        out_specs=[pl.BlockSpec(memory_space=pltpu.VMEM)] * 2,
        out_shape=[pltpu.VMEM(grad.shape, BF16), pltpu.VMEM(lower.shape, BF16)],
        scratch_shapes=[
            pltpu.VMEM((num_rows, num_cols), BF16),
            pltpu.VMEM((num_rows, num_cols), BF16),
            pltpu.VMEM((num_rows, num_cols), BF16),
            pltpu.VMEM((BLK, num_cols), F32),
            pltpu.VMEM((4, 4 * BLK, BLK), BF16),
            pltpu.VMEM((4, 4 * BLK, BLK), BF16),
            pltpu.VMEM((NUM_SLOTS, 2, BLK, BLK), F32),
            pltpu.VMEM((NUM_SLOTS, 2, BLK, BLK), F32),
            pltpu.VMEM((NUM_SLOTS, BLK, BLK), F32),
            pltpu.VMEM((len(FAR_SLOTS), BLK, BLK), BF16),
            pltpu.VMEM((3, BLK, BLK), F32),
            dma((num_bulk,)), dma((num_bulk,)), dma((8,)), dma((6,)), dma((4,)), dma((8,)), dma((4,)), dma((8,)), dma((2,)),
            dma((4,)), dma((4,)), dma((4,)), dma((4,)), dma((5,)), dma((5,)), dma((2,)), dma((2,)),
        ],
        compiler_params=pltpu.CompilerParams(collective_id=0, has_side_effects=True, vmem_limit_bytes=54 * 1024 * 1024),
    )(lower, side, grad)


def solution(mesh):
    spec = P(("batch", "row"), "col")
    return jax.shard_map(per_device, mesh=mesh, in_specs=(spec, spec, spec), out_specs=(spec, spec), check_vma=False)
```

```python
import jax
import jax.numpy as jnp
from jax import lax
from jax.experimental import pallas as pl
from jax.experimental.pallas import tpu as pltpu
from jax.sharding import PartitionSpec as P

BLK = 256
F32 = jnp.float32
BF16 = jnp.bfloat16
MESH = pl.DeviceIdType.MESH
TILE = 512
EARLY = ((0, 2048),)
LATE = ((2048, 1024), (3072, 512), (3584, 512))
CHUNKS = EARLY + LATE
LOCAL_SLOTS = ((0, 0), (1, 0), (2, 0), (3, 0), (2, 1), (3, 1))
FAR_SLOTS = ((3, 0), (3, 1), (2, 0), (2, 1), (1, 0))
NUM_LOCAL = len(LOCAL_SLOTS)
NUM_SLOTS = NUM_LOCAL + len(FAR_SLOTS)
GROUPS = ((0, 6), (6, 8), (8, 10), (10, 11))


def rows(p, n=1):
    return pl.ds(p * BLK, n * BLK)


def kernel(lower, side, grad, db, dl, xr, xl, bl, acc, wl, wr, relay, part, peer, cross, done, corner,
           bulk_s, bulk_r, load_s, wl_s, wl_r, near_s, near_r, far_s, far_r, relay_s, relay_r, push_s, push_r, cross_s, cross_r, back_s, back_r, corner_s, corner_r):
    r = lax.axis_index("row")
    c = lax.axis_index("col")
    x = c // 2
    core = c % 2
    own = core == r
    other = core != r
    across = {"row": 1 - r}
    mate = {"col": 2 * x + 1 - core}
    next_chip = {"col": 2 * (1 - x) + core}
    diagonal = {"col": 2 * (1 - x) + 1 - core}
    num_cols = grad.shape[1]
    sent = []

    def copy_to(device, src, dst, send_sem, recv_sem):
        return pltpu.make_async_remote_copy(src_ref=src, dst_ref=dst, send_sem=send_sem, recv_sem=recv_sem, device_id=device, device_id_type=MESH)

    def start(when, copy):
        sent.append((when, copy))
        if when is None:
            copy.start()
        else:
            pl.when(when)(copy.start)

    def arrived(ref, sem):
        pltpu.make_async_copy(ref, ref, sem).wait()

    barrier = pltpu.get_barrier_semaphore()
    for device in (across, mate, next_chip, diagonal):
        pl.semaphore_signal(barrier, inc=1, device_id=device, device_id_type=MESH)
    pl.semaphore_wait(barrier, 4)

    near_src = (lower.at[pl.ds(BLK, 3 * BLK), pl.ds(0, BLK)], lower.at[pl.ds(3 * BLK, BLK), pl.ds(BLK, BLK)])
    far_src = (lower.at[pl.ds(0, BLK), pl.ds(0, BLK)], lower.at[pl.ds(2 * BLK, BLK), pl.ds(BLK, BLK)])

    def near_dst(q, h):
        return wr.at[q, rows(1, 3)] if h == 0 else wr.at[q, rows(3)]

    def far_dst(q):
        return wr.at[q, rows(q)]

    for h in range(2):
        start(other, copy_to(across, near_src[h], near_dst(x + 2 * h, h), near_s.at[h], near_r.at[x + 2 * h]))
    far_sender = other & (r == 1) & (x == 0)
    for h in range(2):
        start(far_sender, copy_to(next_chip, far_src[h], relay.at[h], far_s.at[h], relay_r.at[h]))

    def bulk(i, p):
        return copy_to(across, grad.at[rows(p)], xr.at[rows(p)], bulk_s.at[i], bulk_r.at[i])

    start(None, bulk(0, 3))

    loads = [pltpu.make_async_copy(side.at[rows(q)], bl.at[rows(q)], load_s.at[q]) for q in range(4)]
    loads += [pltpu.make_async_copy(grad.at[rows(p)], xl.at[rows(p)], load_s.at[4 + p]) for p in range(4)]
    for load in loads:
        load.start()

    for h in range(2):
        src = lower.at[:, pl.ds(0, BLK)] if h == 0 else lower.at[rows(2, 2), pl.ds(BLK, BLK)]
        q = x + 2 * h
        dst = wl.at[q] if h == 0 else wl.at[q, rows(2, 2)]
        pl.when(own)(pltpu.make_async_copy(src, dst, wl_r.at[q]).start)
        for n, device in enumerate((mate, next_chip, diagonal)):
            start(own, copy_to(device, src, dst, wl_s.at[3 * h + n], wl_r.at[q]))

    @pl.when(r == 1)
    def _():
        wr[2, rows(2)] = jnp.zeros((BLK, BLK), BF16)

    for p in range(4):
        for h in range(2):
            far_zero = (x + 2 * h > p + r - 1) if p else (x >= 0)
            zero = (other & far_zero) | (own & (x + 2 * h > p))

            @pl.when(zero)
            def _():
                dl[rows(p), rows(h)] = jnp.zeros((BLK, BLK), BF16)

    def outer(left, left_row, q):
        total = None
        for k in range(0, num_cols, 1024):
            term = lax.dot_general(left[pl.ds(left_row, BLK), pl.ds(k, 1024)], bl[pl.ds(q * BLK, BLK), pl.ds(k, 1024)], (((1,), (1,)), ((), ())), preferred_element_type=F32)
            total = term if total is None else total + term
        return total

    for load in loads:
        load.wait()

    def local_outer(i, carry):
        slot, parity = i // 2, i % 2
        h = slot // 4
        p = slot - 2 * h
        part[slot, parity] = outer(xl, pl.multiple_of(p * BLK, BLK), 2 * h + parity)
        return carry

    lax.fori_loop(0, 2 * NUM_LOCAL, local_outer, 0)

    for h in range(2):
        q = x + 2 * h

        @pl.when(own)
        def _():
            arrived(near_dst(q, h), near_r.at[q])

        for n, device in enumerate((mate, next_chip, diagonal)):
            start(own, copy_to(device, near_dst(q, h), near_dst(q, h), near_s.at[2 + 3 * h + n], near_r.at[q]))
    far_owner = own & (r == 0) & (x == 1)
    relay_here = other & (r == 1) & (x == 1)
    for h in range(2):

        @pl.when(relay_here)
        def _():
            arrived(relay.at[h], relay_r.at[h])

        start(relay_here, copy_to(across, relay.at[h], far_dst(2 * h), relay_s.at[h], far_r.at[h]))
    start(None, bulk(1, 2))

    def push(g):
        lo, hi = GROUPS[g]
        span = pl.ds(lo, hi - lo)
        start(other, copy_to(mate, part.at[span], peer.at[span], push_s.at[g], push_r.at[g]))

    def add_and_cross(g):
        lo, hi = GROUPS[g]
        span = pl.ds(lo, hi - lo)

        @pl.when(own)
        def _():
            arrived(peer.at[span], push_r.at[g])

            def add(slot, carry):
                part[slot] = part[slot] + peer[slot]
                return carry

            lax.fori_loop(lo, hi, add, 0)

        start(own, copy_to(next_chip, part.at[span, 1 - x], cross.at[span], cross_s.at[g], cross_r.at[g]))

    def wait_cross(g):
        lo, hi = GROUPS[g]
        arrived(cross.at[pl.ds(lo, hi - lo)], cross_r.at[g])

    def back_copies(i):
        p, h = FAR_SLOTS[i]
        return copy_to(across, done.at[i], dl.at[rows(p), rows(h)], back_s.at[i], back_r.at[i])

    def finish_far(g):
        lo, hi = GROUPS[g]

        @pl.when(own)
        def _():
            wait_cross(g)
            for slot in range(lo, hi):
                done[slot - NUM_LOCAL] = (part[slot, x] + cross[slot]).astype(BF16)

        for slot in range(lo, hi):
            p, h = FAR_SLOTS[slot - NUM_LOCAL]
            start(own & (x + 2 * h <= p - r), back_copies(slot - NUM_LOCAL))

    def finish_local():
        @pl.when(own)
        def _():
            wait_cross(0)
            below = lax.broadcasted_iota(jnp.int32, (BLK, BLK), 0) >= lax.broadcasted_iota(jnp.int32, (BLK, BLK), 1)
            for slot, (p, h) in enumerate(LOCAL_SLOTS):
                q = x + 2 * h

                @pl.when(q <= p)
                def _():
                    total = part[slot, x] + cross[slot]
                    keep = below | (q < p)
                    dl[rows(p), rows(h)] = jnp.where(keep, total, 0.0).astype(BF16)

    def far_outer(p, lo, num_q):
        def body(q, carry):
            part[lo + q // 2, q % 2] = outer(xr, p * BLK, q)
            return carry

        lax.fori_loop(0, num_q, body, 0)

    def row_sum(q, far_first, cols):
        near = lax.dot_general(wl[q, rows(q, 4 - q)], xl[rows(q, 4 - q), cols], (((0,), (0,)), ((), ())), preferred_element_type=F32)
        far = lax.dot_general(wr[q, rows(far_first, 4 - far_first)], xr[rows(far_first, 4 - far_first), cols], (((0,), (0,)), ((), ())), preferred_element_type=F32)
        return near + far

    def tile_loop(body):
        def step(j, carry):
            body(pl.ds(pl.multiple_of(j * TILE, TILE), TILE))
            return carry

        lax.fori_loop(0, num_cols // TILE, step, 0)

    def weights_here(q):
        h = q // 2
        arrived(wl.at[q] if h == 0 else wl.at[q, rows(2, 2)], wl_r.at[q])
        if h == 0:
            pl.when(other | (x != q))(lambda: arrived(near_dst(q, h), near_r.at[q]))
        else:
            pl.when(other | (x + 2 != q))(lambda: arrived(near_dst(q, h), near_r.at[q]))
        if q % 2 == 0:
            pl.when((r == 0) & jnp.logical_not(far_owner))(lambda: arrived(far_dst(q), far_r.at[h]))

    def block_row(q):
        weights_here(q)

        def body(cols):
            db[rows(q), cols] = row_sum(q, q, cols).astype(BF16)

        tile_loop(body)

    def chunk_copy(i, source):
        first, width = CHUNKS[i]
        cols = pl.ds(first, width)
        sems = bulk_s.at[3 + i], bulk_r.at[3 + i]
        return copy_to(across, source.at[rows(0), cols], xr.at[rows(0), cols], *sems)

    def start_chunks(when, span):
        for i in span:
            start(when & (r == 1), chunk_copy(i, grad))
            if CHUNKS[i] in LATE:
                start(when & (r == 0), chunk_copy(i, side))

    arrived(xr.at[rows(3)], bulk_r.at[0])
    push(0)
    far_outer(3, 6, 4)
    block_row(3)
    start(None, bulk(2, 1))
    for h in range(2):

        @pl.when(far_owner)
        def _():
            arrived(far_dst(2 * h), far_r.at[h])

        for n, device in enumerate((mate, next_chip, diagonal)):
            start(far_owner, copy_to(device, far_dst(2 * h), far_dst(2 * h), far_s.at[2 + 3 * h + n], far_r.at[h]))
    push(1)
    add_and_cross(0)
    add_and_cross(1)

    arrived(xr.at[rows(2)], bulk_r.at[1])
    finish_far(1)
    early = range(len(EARLY))
    late = range(len(EARLY), len(CHUNKS))
    start_chunks(core >= 0, early)
    far_outer(2, 8, 4)
    block_row(2)
    push(2)
    finish_local()
    add_and_cross(2)

    arrived(xr.at[rows(1)], bulk_r.at[2])
    last_sender = own & (r == 1)
    start_chunks(jnp.logical_not(last_sender), late)
    finish_far(2)
    far_outer(1, 10, 2)
    block_row(1)
    push(3)
    weights_here(0)

    def first_row(cols):
        total = row_sum(0, 1, cols)

        @pl.when(r == 1)
        def _():
            db[rows(0), cols] = total.astype(BF16)

        @pl.when(r == 0)
        def _():
            acc[:, cols] = total

    def first_half(lo, hi):
        def step(j, carry):
            first_row(pl.ds(pl.multiple_of(j * TILE, TILE), TILE))
            return carry

        lax.fori_loop(lo, hi, step, 0)

    add_and_cross(3)
    first_half(0, num_cols // TILE)
    finish_far(3)
    start_chunks(last_sender, late)

    corner[0] = jnp.zeros((BLK, BLK), F32)

    def nt_dot(left, right):
        return lax.dot_general(left, right, (((1,), (1,)), ((), ())), preferred_element_type=F32)

    def corner_in_row(row):
        start((r == row) & (core == 1), copy_to(mate, corner.at[0], corner.at[1], corner_s.at[0], corner_r.at[0]))
        owner = (r == row) & (core == 0)

        @pl.when(owner)
        def _():
            arrived(corner.at[1], corner_r.at[0])
            corner[0] += corner[1]

        start(owner & (x == 1), copy_to(next_chip, corner.at[0], corner.at[2], corner_s.at[1], corner_r.at[1]))

        @pl.when(owner & (x == 0))
        def _():
            arrived(corner.at[2], corner_r.at[1])

        return owner & (x == 0)

    for i, (first, width) in enumerate(CHUNKS):
        early_chunk = (first, width) in EARLY
        here = (r == 0) if early_chunk else (r >= 0)

        @pl.when(here)
        def _():
            arrived(xr.at[rows(0), pl.ds(first, width)], bulk_r.at[3 + i])

            def step(j, carry):
                cols = pl.ds(pl.multiple_of(first + j * TILE, TILE), TILE)

                @pl.when(r == 0)
                def _():
                    term = lax.dot_general(wr[0, rows(0)], xr[rows(0), cols], (((0,), (0,)), ((), ())), preferred_element_type=F32)
                    db[rows(0), cols] = (acc[:, cols] + term).astype(BF16)
                    if early_chunk:
                        corner[0] += nt_dot(xr[rows(0), cols], bl[rows(0), cols])

                if not early_chunk:

                    @pl.when(r == 1)
                    def _():
                        corner[0] += nt_dot(xl[rows(0), cols], xr[rows(0), cols])

                return carry

            lax.fori_loop(0, width // TILE, step, 0)

        if i == len(EARLY) - 1:
            first_device = corner_in_row(0)

            @pl.when(first_device)
            def _():
                corner[0] += corner[2]

            start(first_device, copy_to(across, corner.at[0], corner.at[3], corner_s.at[2], corner_r.at[2]))

    last_device = corner_in_row(1)

    @pl.when(last_device)
    def _():
        arrived(corner.at[3], corner_r.at[2])
        dl[rows(0), rows(0)] = (corner[0] + corner[2] + corner[3]).astype(BF16)

    for i, (p, h) in enumerate(FAR_SLOTS):
        pl.when(other & (x + 2 * h <= p + r - 1))(lambda: arrived(dl.at[rows(p), rows(h)], back_r.at[i]))
    for when, copy in sent:
        if when is None:
            copy.wait_send()
        else:
            pl.when(when)(copy.wait_send)


def per_device(lower, side, grad):
    num_rows, num_cols = grad.shape
    dma = pltpu.SemaphoreType.DMA
    num_bulk = 3 + len(CHUNKS)
    return pl.pallas_call(
        kernel,
        in_specs=[pl.BlockSpec(memory_space=pl.ANY)] * 3,
        out_specs=[pl.BlockSpec(memory_space=pltpu.VMEM)] * 2,
        out_shape=[pltpu.VMEM(grad.shape, BF16), pltpu.VMEM(lower.shape, BF16)],
        scratch_shapes=[
            pltpu.VMEM((num_rows, num_cols), BF16),
            pltpu.VMEM((num_rows, num_cols), BF16),
            pltpu.VMEM((num_rows, num_cols), BF16),
            pltpu.VMEM((BLK, num_cols), F32),
            pltpu.VMEM((4, 4 * BLK, BLK), BF16),
            pltpu.VMEM((4, 4 * BLK, BLK), BF16),
            pltpu.VMEM((2, BLK, BLK), BF16),
            pltpu.VMEM((NUM_SLOTS, 2, BLK, BLK), F32),
            pltpu.VMEM((NUM_SLOTS, 2, BLK, BLK), F32),
            pltpu.VMEM((NUM_SLOTS, BLK, BLK), F32),
            pltpu.VMEM((len(FAR_SLOTS), BLK, BLK), BF16),
            pltpu.VMEM((4, BLK, BLK), F32),
            dma((num_bulk,)), dma((num_bulk,)), dma((8,)), dma((6,)), dma((4,)), dma((8,)), dma((4,)), dma((8,)), dma((2,)), dma((2,)), dma((2,)),
            dma((4,)), dma((4,)), dma((4,)), dma((4,)), dma((5,)), dma((5,)), dma((3,)), dma((3,)),
        ],
        compiler_params=pltpu.CompilerParams(collective_id=0, has_side_effects=True, vmem_limit_bytes=54 * 1024 * 1024),
    )(lower, side, grad)


def solution(mesh):
    spec = P(("batch", "row"), "col")
    return jax.shard_map(per_device, mesh=mesh, in_specs=(spec, spec, spec), out_specs=(spec, spec), check_vma=False)
```

```python
import jax
import jax.numpy as jnp
from jax import lax
from jax.experimental import pallas as pl
from jax.experimental.pallas import tpu as pltpu
from jax.sharding import PartitionSpec as P

BLK = 256
F32 = jnp.float32
BF16 = jnp.bfloat16
MESH = pl.DeviceIdType.MESH
TILE = 512
EARLY = ((0, 2048),)
LATE = ((2048, 1024), (3072, 512), (3584, 512))
CHUNKS = EARLY + LATE
LOCAL_SLOTS = ((0, 0), (1, 0), (2, 0), (3, 0), (2, 1), (3, 1))
FAR_SLOTS = ((3, 0), (3, 1), (2, 0), (2, 1), (1, 0))
NUM_LOCAL = len(LOCAL_SLOTS)
NUM_SLOTS = NUM_LOCAL + len(FAR_SLOTS)
GROUPS = ((0, 6), (6, 8), (8, 10), (10, 11))


def rows(p, n=1):
    return pl.ds(p * BLK, n * BLK)


def kernel(lower, side, grad, db, dl, xr, xl, bl, acc, wl, wr, relay, part, peer, cross, done, corner,
           bulk_s, bulk_r, load_s, wl_s, wl_r, near_s, near_r, far_s, far_r, relay_s, relay_r, push_s, push_r, cross_s, cross_r, back_s, back_r, corner_s, corner_r):
    r = lax.axis_index("row")
    c = lax.axis_index("col")
    x = c // 2
    core = c % 2
    own = core == r
    other = core != r
    across = {"row": 1 - r}
    mate = {"col": 2 * x + 1 - core}
    next_chip = {"col": 2 * (1 - x) + core}
    diagonal = {"col": 2 * (1 - x) + 1 - core}
    num_cols = grad.shape[1]
    sent = []

    def copy_to(device, src, dst, send_sem, recv_sem):
        return pltpu.make_async_remote_copy(src_ref=src, dst_ref=dst, send_sem=send_sem, recv_sem=recv_sem, device_id=device, device_id_type=MESH)

    def start(when, copy):
        sent.append((when, copy))
        if when is None:
            copy.start()
        else:
            pl.when(when)(copy.start)

    def arrived(ref, sem):
        pltpu.make_async_copy(ref, ref, sem).wait()

    barrier = pltpu.get_barrier_semaphore()

    def greet(when, *devices):
        @pl.when(when)
        def _():
            for device in devices:
                pl.semaphore_signal(barrier, inc=1, device_id=device, device_id_type=MESH)

    first_core = core == 0
    second_core = core == 1
    greet(first_core, across)
    greet(second_core, across, next_chip)
    pl.when(first_core)(lambda: pl.semaphore_wait(barrier, 1))

    near_src = (lower.at[pl.ds(BLK, 3 * BLK), pl.ds(0, BLK)], lower.at[pl.ds(3 * BLK, BLK), pl.ds(BLK, BLK)])
    far_src = (lower.at[pl.ds(0, BLK), pl.ds(0, BLK)], lower.at[pl.ds(2 * BLK, BLK), pl.ds(BLK, BLK)])

    def near_dst(q, h):
        return wr.at[q, rows(1, 3)] if h == 0 else wr.at[q, rows(3)]

    def far_dst(q):
        return wr.at[q, rows(q)]

    def bulk(i, p):
        return copy_to(across, grad.at[rows(p)], xr.at[rows(p)], bulk_s.at[i], bulk_r.at[i])

    def first_copies(when):
        for h in range(2):
            start(when & other, copy_to(across, near_src[h], near_dst(x + 2 * h, h), near_s.at[h], near_r.at[x + 2 * h]))
        start(when, bulk(0, 3))

    first_copies(first_core)
    greet(first_core, mate, diagonal)
    pl.when(second_core)(lambda: pl.semaphore_wait(barrier, 4))
    first_copies(second_core)
    greet(second_core, mate)
    pl.when(first_core)(lambda: pl.semaphore_wait(barrier, 1))

    far_sender = other & (r == 1) & (x == 0)
    for h in range(2):
        start(far_sender, copy_to(next_chip, far_src[h], relay.at[h], far_s.at[h], relay_r.at[h]))

    loads = [pltpu.make_async_copy(side.at[rows(q)], bl.at[rows(q)], load_s.at[q]) for q in range(4)]
    loads += [pltpu.make_async_copy(grad.at[rows(p)], xl.at[rows(p)], load_s.at[4 + p]) for p in range(4)]
    for load in loads:
        load.start()

    for h in range(2):
        src = lower.at[:, pl.ds(0, BLK)] if h == 0 else lower.at[rows(2, 2), pl.ds(BLK, BLK)]
        q = x + 2 * h
        dst = wl.at[q] if h == 0 else wl.at[q, rows(2, 2)]
        pl.when(own)(pltpu.make_async_copy(src, dst, wl_r.at[q]).start)
        for n, device in enumerate((mate, next_chip, diagonal)):
            start(own, copy_to(device, src, dst, wl_s.at[3 * h + n], wl_r.at[q]))

    @pl.when(r == 1)
    def _():
        wr[2, rows(2)] = jnp.zeros((BLK, BLK), BF16)

    for p in range(4):
        for h in range(2):
            far_zero = (x + 2 * h > p + r - 1) if p else (x >= 0)
            zero = (other & far_zero) | (own & (x + 2 * h > p))

            @pl.when(zero)
            def _():
                dl[rows(p), rows(h)] = jnp.zeros((BLK, BLK), BF16)

    def outer(left, left_row, q):
        total = None
        for k in range(0, num_cols, 1024):
            term = lax.dot_general(left[pl.ds(left_row, BLK), pl.ds(k, 1024)], bl[pl.ds(q * BLK, BLK), pl.ds(k, 1024)], (((1,), (1,)), ((), ())), preferred_element_type=F32)
            total = term if total is None else total + term
        return total

    for load in loads:
        load.wait()

    def local_outer(i, carry):
        slot, parity = i // 2, i % 2
        h = slot // 4
        p = slot - 2 * h
        part[slot, parity] = outer(xl, pl.multiple_of(p * BLK, BLK), 2 * h + parity)
        return carry

    lax.fori_loop(0, 2 * NUM_LOCAL, local_outer, 0)

    for h in range(2):
        q = x + 2 * h

        @pl.when(own)
        def _():
            arrived(near_dst(q, h), near_r.at[q])

        for n, device in enumerate((mate, next_chip, diagonal)):
            start(own, copy_to(device, near_dst(q, h), near_dst(q, h), near_s.at[2 + 3 * h + n], near_r.at[q]))
    far_owner = own & (r == 0) & (x == 1)
    relay_here = other & (r == 1) & (x == 1)
    for h in range(2):

        @pl.when(relay_here)
        def _():
            arrived(relay.at[h], relay_r.at[h])

        start(relay_here, copy_to(across, relay.at[h], far_dst(2 * h), relay_s.at[h], far_r.at[h]))
    start(None, bulk(1, 2))

    def push(g):
        lo, hi = GROUPS[g]
        span = pl.ds(lo, hi - lo)
        start(other, copy_to(mate, part.at[span], peer.at[span], push_s.at[g], push_r.at[g]))

    def add_and_cross(g):
        lo, hi = GROUPS[g]
        span = pl.ds(lo, hi - lo)

        @pl.when(own)
        def _():
            arrived(peer.at[span], push_r.at[g])

            def add(slot, carry):
                part[slot] = part[slot] + peer[slot]
                return carry

            lax.fori_loop(lo, hi, add, 0)

        start(own, copy_to(next_chip, part.at[span, 1 - x], cross.at[span], cross_s.at[g], cross_r.at[g]))

    def wait_cross(g):
        lo, hi = GROUPS[g]
        arrived(cross.at[pl.ds(lo, hi - lo)], cross_r.at[g])

    def back_copies(i):
        p, h = FAR_SLOTS[i]
        return copy_to(across, done.at[i], dl.at[rows(p), rows(h)], back_s.at[i], back_r.at[i])

    def finish_far(g):
        lo, hi = GROUPS[g]

        @pl.when(own)
        def _():
            wait_cross(g)
            for slot in range(lo, hi):
                done[slot - NUM_LOCAL] = (part[slot, x] + cross[slot]).astype(BF16)

        for slot in range(lo, hi):
            p, h = FAR_SLOTS[slot - NUM_LOCAL]
            start(own & (x + 2 * h <= p - r), back_copies(slot - NUM_LOCAL))

    def finish_local():
        @pl.when(own)
        def _():
            wait_cross(0)
            below = lax.broadcasted_iota(jnp.int32, (BLK, BLK), 0) >= lax.broadcasted_iota(jnp.int32, (BLK, BLK), 1)
            for slot, (p, h) in enumerate(LOCAL_SLOTS):
                q = x + 2 * h

                @pl.when(q <= p)
                def _():
                    total = part[slot, x] + cross[slot]
                    keep = below | (q < p)
                    dl[rows(p), rows(h)] = jnp.where(keep, total, 0.0).astype(BF16)

    def far_outer(p, lo, num_q):
        def body(q, carry):
            part[lo + q // 2, q % 2] = outer(xr, p * BLK, q)
            return carry

        lax.fori_loop(0, num_q, body, 0)

    def row_sum(q, far_first, cols):
        near = lax.dot_general(wl[q, rows(q, 4 - q)], xl[rows(q, 4 - q), cols], (((0,), (0,)), ((), ())), preferred_element_type=F32)
        far = lax.dot_general(wr[q, rows(far_first, 4 - far_first)], xr[rows(far_first, 4 - far_first), cols], (((0,), (0,)), ((), ())), preferred_element_type=F32)
        return near + far

    def tile_loop(body):
        def step(j, carry):
            body(pl.ds(pl.multiple_of(j * TILE, TILE), TILE))
            return carry

        lax.fori_loop(0, num_cols // TILE, step, 0)

    def weights_here(q):
        h = q // 2
        arrived(wl.at[q] if h == 0 else wl.at[q, rows(2, 2)], wl_r.at[q])
        if h == 0:
            pl.when(other | (x != q))(lambda: arrived(near_dst(q, h), near_r.at[q]))
        else:
            pl.when(other | (x + 2 != q))(lambda: arrived(near_dst(q, h), near_r.at[q]))
        if q % 2 == 0:
            pl.when((r == 0) & jnp.logical_not(far_owner))(lambda: arrived(far_dst(q), far_r.at[h]))

    def block_row(q):
        weights_here(q)

        def body(cols):
            db[rows(q), cols] = row_sum(q, q, cols).astype(BF16)

        tile_loop(body)

    def chunk_copy(i, source):
        first, width = CHUNKS[i]
        cols = pl.ds(first, width)
        sems = bulk_s.at[3 + i], bulk_r.at[3 + i]
        return copy_to(across, source.at[rows(0), cols], xr.at[rows(0), cols], *sems)

    def start_chunks(when, span):
        for i in span:
            start(when & (r == 1), chunk_copy(i, grad))
            if CHUNKS[i] in LATE:
                start(when & (r == 0), chunk_copy(i, side))

    arrived(xr.at[rows(3)], bulk_r.at[0])
    push(0)
    far_outer(3, 6, 4)
    block_row(3)
    start(None, bulk(2, 1))
    for h in range(2):

        @pl.when(far_owner)
        def _():
            arrived(far_dst(2 * h), far_r.at[h])

        for n, device in enumerate((mate, next_chip, diagonal)):
            start(far_owner, copy_to(device, far_dst(2 * h), far_dst(2 * h), far_s.at[2 + 3 * h + n], far_r.at[h]))
    push(1)
    add_and_cross(0)
    add_and_cross(1)

    arrived(xr.at[rows(2)], bulk_r.at[1])
    finish_far(1)
    early = range(len(EARLY))
    late = range(len(EARLY), len(CHUNKS))
    start_chunks(core >= 0, early)
    far_outer(2, 8, 4)
    block_row(2)
    push(2)
    finish_local()
    add_and_cross(2)

    arrived(xr.at[rows(1)], bulk_r.at[2])
    last_sender = own & (r == 1)
    start_chunks(jnp.logical_not(last_sender), late)
    finish_far(2)
    far_outer(1, 10, 2)
    block_row(1)
    push(3)
    weights_here(0)

    def first_row(cols):
        total = row_sum(0, 1, cols)

        @pl.when(r == 1)
        def _():
            db[rows(0), cols] = total.astype(BF16)

        @pl.when(r == 0)
        def _():
            acc[:, cols] = total

    def first_half(lo, hi):
        def step(j, carry):
            first_row(pl.ds(pl.multiple_of(j * TILE, TILE), TILE))
            return carry

        lax.fori_loop(lo, hi, step, 0)

    add_and_cross(3)
    first_half(0, num_cols // TILE)
    finish_far(3)
    start_chunks(last_sender, late)

    corner[0] = jnp.zeros((BLK, BLK), F32)

    def nt_dot(left, right):
        return lax.dot_general(left, right, (((1,), (1,)), ((), ())), preferred_element_type=F32)

    def corner_in_row(row):
        start((r == row) & (core == 1), copy_to(mate, corner.at[0], corner.at[1], corner_s.at[0], corner_r.at[0]))
        owner = (r == row) & (core == 0)

        @pl.when(owner)
        def _():
            arrived(corner.at[1], corner_r.at[0])
            corner[0] += corner[1]

        start(owner & (x == 1), copy_to(next_chip, corner.at[0], corner.at[2], corner_s.at[1], corner_r.at[1]))

        @pl.when(owner & (x == 0))
        def _():
            arrived(corner.at[2], corner_r.at[1])

        return owner & (x == 0)

    for i, (first, width) in enumerate(CHUNKS):
        early_chunk = (first, width) in EARLY
        here = (r == 0) if early_chunk else (r >= 0)

        @pl.when(here)
        def _():
            arrived(xr.at[rows(0), pl.ds(first, width)], bulk_r.at[3 + i])

            def step(j, carry):
                cols = pl.ds(pl.multiple_of(first + j * TILE, TILE), TILE)

                @pl.when(r == 0)
                def _():
                    term = lax.dot_general(wr[0, rows(0)], xr[rows(0), cols], (((0,), (0,)), ((), ())), preferred_element_type=F32)
                    db[rows(0), cols] = (acc[:, cols] + term).astype(BF16)
                    if early_chunk:
                        corner[0] += nt_dot(xr[rows(0), cols], bl[rows(0), cols])

                if not early_chunk:

                    @pl.when(r == 1)
                    def _():
                        corner[0] += nt_dot(xl[rows(0), cols], xr[rows(0), cols])

                return carry

            lax.fori_loop(0, width // TILE, step, 0)

        if i == len(EARLY) - 1:
            first_device = corner_in_row(0)

            @pl.when(first_device)
            def _():
                corner[0] += corner[2]

            start(first_device, copy_to(across, corner.at[0], corner.at[3], corner_s.at[2], corner_r.at[2]))

    last_device = corner_in_row(1)

    @pl.when(last_device)
    def _():
        arrived(corner.at[3], corner_r.at[2])
        dl[rows(0), rows(0)] = (corner[0] + corner[2] + corner[3]).astype(BF16)

    for i, (p, h) in enumerate(FAR_SLOTS):
        pl.when(other & (x + 2 * h <= p + r - 1))(lambda: arrived(dl.at[rows(p), rows(h)], back_r.at[i]))
    for when, copy in sent:
        if when is None:
            copy.wait_send()
        else:
            pl.when(when)(copy.wait_send)


def per_device(lower, side, grad):
    num_rows, num_cols = grad.shape
    dma = pltpu.SemaphoreType.DMA
    num_bulk = 3 + len(CHUNKS)
    results = pl.pallas_call(
        kernel,
        in_specs=[pl.BlockSpec(memory_space=pl.ANY)] * 3,
        out_specs=[pl.BlockSpec(memory_space=pltpu.VMEM)] * 2,
        out_shape=[pltpu.VMEM(grad.shape, BF16), pltpu.VMEM(lower.shape, BF16)],
        scratch_shapes=[
            pltpu.VMEM((num_rows, num_cols), BF16),
            pltpu.VMEM((num_rows, num_cols), BF16),
            pltpu.VMEM((num_rows, num_cols), BF16),
            pltpu.VMEM((BLK, num_cols), F32),
            pltpu.VMEM((4, 4 * BLK, BLK), BF16),
            pltpu.VMEM((4, 4 * BLK, BLK), BF16),
            pltpu.VMEM((2, BLK, BLK), BF16),
            pltpu.VMEM((NUM_SLOTS, 2, BLK, BLK), F32),
            pltpu.VMEM((NUM_SLOTS, 2, BLK, BLK), F32),
            pltpu.VMEM((NUM_SLOTS, BLK, BLK), F32),
            pltpu.VMEM((len(FAR_SLOTS), BLK, BLK), BF16),
            pltpu.VMEM((4, BLK, BLK), F32),
            dma((num_bulk,)), dma((num_bulk,)), dma((8,)), dma((6,)), dma((4,)), dma((8,)), dma((4,)), dma((8,)), dma((2,)), dma((2,)), dma((2,)),
            dma((4,)), dma((4,)), dma((4,)), dma((4,)), dma((5,)), dma((5,)), dma((3,)), dma((3,)),
        ],
        compiler_params=pltpu.CompilerParams(collective_id=0, has_side_effects=True, vmem_limit_bytes=54 * 1024 * 1024),
    )(lower, side, grad)
    pieces = 4
    return pl.pallas_call(
        put_kernel,
        in_specs=[pl.BlockSpec(memory_space=pltpu.VMEM)] * 2,
        out_specs=[pl.BlockSpec(memory_space=pl.ANY)] * 2,
        out_shape=[jax.ShapeDtypeStruct(grad.shape, BF16), jax.ShapeDtypeStruct(lower.shape, BF16)],
        scratch_shapes=[dma((pieces + 1,))],
        compiler_params=pltpu.CompilerParams(vmem_limit_bytes=1024 * 1024),
    )(*[pltpu.with_memory_space_constraint(v, pltpu.VMEM) for v in results])


def put_kernel(db_in, dl_in, db_out, dl_out, sems):
    copies = [pltpu.make_async_copy(dl_in, dl_out, sems.at[0])]
    copies += [pltpu.make_async_copy(db_in.at[rows(i)], db_out.at[rows(i)], sems.at[1 + i]) for i in range(4)]
    for copy in copies:
        copy.start()
    for copy in copies:
        copy.wait()


def solution(mesh):
    spec = P(("batch", "row"), "col")
    return jax.shard_map(per_device, mesh=mesh, in_specs=(spec, spec, spec), out_specs=(spec, spec), check_vma=False)
```

```python
import jax
import jax.numpy as jnp
from jax import lax
from jax.experimental import pallas as pl
from jax.experimental.pallas import tpu as pltpu
from jax.sharding import PartitionSpec as P

BLK = 256
F32 = jnp.float32
BF16 = jnp.bfloat16
MESH = pl.DeviceIdType.MESH
TILE = 512
EARLY = ((0, 2048),)
LATE = ((2048, 1024), (3072, 512), (3584, 512))
CHUNKS = EARLY + LATE
LOCAL_SLOTS = ((0, 0), (1, 0), (2, 0), (3, 0), (2, 1), (3, 1))
FAR_SLOTS = ((3, 0), (3, 1), (2, 0), (2, 1), (1, 0))
NUM_LOCAL = len(LOCAL_SLOTS)
NUM_SLOTS = NUM_LOCAL + len(FAR_SLOTS)
GROUPS = ((0, 6), (6, 8), (8, 10), (10, 11))


def rows(p, n=1):
    return pl.ds(p * BLK, n * BLK)


def kernel(lower, side, grad, db, dl, acc, corner_weight, xr, xl, bl, wl, wr, relay, part, peer, cross, done, corner,
           bulk_s, bulk_r, load_s, wl_s, wl_r, near_s, near_r, far_s, far_r, relay_s, relay_r, push_s, push_r, cross_s, cross_r, back_s, back_r, corner_s, corner_r):
    r = lax.axis_index("row")
    c = lax.axis_index("col")
    x = c // 2
    core = c % 2
    own = core == r
    other = core != r
    across = {"row": 1 - r}
    mate = {"col": 2 * x + 1 - core}
    next_chip = {"col": 2 * (1 - x) + core}
    diagonal = {"col": 2 * (1 - x) + 1 - core}
    num_cols = grad.shape[1]
    sent = []

    def copy_to(device, src, dst, send_sem, recv_sem):
        return pltpu.make_async_remote_copy(src_ref=src, dst_ref=dst, send_sem=send_sem, recv_sem=recv_sem, device_id=device, device_id_type=MESH)

    def start(when, copy):
        sent.append((when, copy))
        if when is None:
            copy.start()
        else:
            pl.when(when)(copy.start)

    def arrived(ref, sem):
        pltpu.make_async_copy(ref, ref, sem).wait()

    barrier = pltpu.get_barrier_semaphore()

    def greet(when, *devices):
        @pl.when(when)
        def _():
            for device in devices:
                pl.semaphore_signal(barrier, inc=1, device_id=device, device_id_type=MESH)

    first_core = core == 0
    second_core = core == 1
    greet(first_core, across)
    greet(second_core, across, next_chip)
    pl.when(first_core)(lambda: pl.semaphore_wait(barrier, 1))

    near_src = (lower.at[pl.ds(BLK, 3 * BLK), pl.ds(0, BLK)], lower.at[pl.ds(3 * BLK, BLK), pl.ds(BLK, BLK)])
    far_src = (lower.at[pl.ds(0, BLK), pl.ds(0, BLK)], lower.at[pl.ds(2 * BLK, BLK), pl.ds(BLK, BLK)])

    def near_dst(q, h):
        return wr.at[q, rows(1, 3)] if h == 0 else wr.at[q, rows(3)]

    def far_dst(q):
        return wr.at[q, rows(q)]

    def bulk(i, p):
        return copy_to(across, grad.at[rows(p)], xr.at[rows(p)], bulk_s.at[i], bulk_r.at[i])

    def first_copies(when):
        for h in range(2):
            start(when & other, copy_to(across, near_src[h], near_dst(x + 2 * h, h), near_s.at[h], near_r.at[x + 2 * h]))
        start(when, bulk(0, 3))

    first_copies(first_core)
    greet(first_core, mate, diagonal)
    pl.when(second_core)(lambda: pl.semaphore_wait(barrier, 4))
    first_copies(second_core)
    greet(second_core, mate)
    pl.when(first_core)(lambda: pl.semaphore_wait(barrier, 1))

    far_sender = other & (r == 1) & (x == 0)
    for h in range(2):
        start(far_sender, copy_to(diagonal, far_src[h], relay.at[h], far_s.at[h], relay_r.at[h]))

    loads = [pltpu.make_async_copy(side.at[rows(q)], bl.at[rows(q)], load_s.at[q]) for q in range(4)]
    loads += [pltpu.make_async_copy(grad.at[rows(p)], xl.at[rows(p)], load_s.at[4 + p]) for p in range(4)]
    for load in loads:
        load.start()

    for h in range(2):
        src = lower.at[:, pl.ds(0, BLK)] if h == 0 else lower.at[rows(2, 2), pl.ds(BLK, BLK)]
        q = x + 2 * h
        dst = wl.at[q] if h == 0 else wl.at[q, rows(2, 2)]
        pl.when(own)(pltpu.make_async_copy(src, dst, wl_r.at[q]).start)
        for n, device in enumerate((mate, next_chip, diagonal)):
            start(own, copy_to(device, src, dst, wl_s.at[3 * h + n], wl_r.at[q]))

    @pl.when(r == 1)
    def _():
        wr[2, rows(2)] = jnp.zeros((BLK, BLK), BF16)

    for p in range(4):
        for h in range(2):
            far_zero = (x + 2 * h > p + r - 1) if p else (x >= 0)
            zero = (other & far_zero) | (own & (x + 2 * h > p))

            @pl.when(zero)
            def _():
                dl[rows(p), rows(h)] = jnp.zeros((BLK, BLK), BF16)

    def outer(left, left_row, q):
        total = None
        for k in range(0, num_cols, 1024):
            term = lax.dot_general(left[pl.ds(left_row, BLK), pl.ds(k, 1024)], bl[pl.ds(q * BLK, BLK), pl.ds(k, 1024)], (((1,), (1,)), ((), ())), preferred_element_type=F32)
            total = term if total is None else total + term
        return total

    for load in loads:
        load.wait()

    def local_outer(i, carry):
        slot, parity = i // 2, i % 2
        h = slot // 4
        p = slot - 2 * h
        part[slot, parity] = outer(xl, pl.multiple_of(p * BLK, BLK), 2 * h + parity)
        return carry

    lax.fori_loop(0, 2 * NUM_LOCAL, local_outer, 0)

    for h in range(2):
        q = x + 2 * h

        @pl.when(own)
        def _():
            arrived(near_dst(q, h), near_r.at[q])

        for n, device in enumerate((mate, next_chip, diagonal)):
            start(own, copy_to(device, near_dst(q, h), near_dst(q, h), near_s.at[2 + 3 * h + n], near_r.at[q]))
    far_owner = other & (r == 0) & (x == 1)
    relay_here = own & (r == 1) & (x == 1)
    for h in range(2):

        @pl.when(relay_here)
        def _():
            arrived(relay.at[h], relay_r.at[h])

        start(relay_here, copy_to(across, relay.at[h], far_dst(2 * h), relay_s.at[h], far_r.at[h]))
    start(None, bulk(1, 2))

    def push(g):
        lo, hi = GROUPS[g]
        span = pl.ds(lo, hi - lo)
        start(other, copy_to(mate, part.at[span], peer.at[span], push_s.at[g], push_r.at[g]))

    def add_and_cross(g):
        lo, hi = GROUPS[g]
        span = pl.ds(lo, hi - lo)

        @pl.when(own)
        def _():
            arrived(peer.at[span], push_r.at[g])

            def add(slot, carry):
                part[slot] = part[slot] + peer[slot]
                return carry

            lax.fori_loop(lo, hi, add, 0)

        start(own, copy_to(next_chip, part.at[span, 1 - x], cross.at[span], cross_s.at[g], cross_r.at[g]))

    def wait_cross(g):
        lo, hi = GROUPS[g]
        arrived(cross.at[pl.ds(lo, hi - lo)], cross_r.at[g])

    def back_copies(i):
        p, h = FAR_SLOTS[i]
        return copy_to(across, done.at[i], dl.at[rows(p), rows(h)], back_s.at[i], back_r.at[i])

    def finish_far(g):
        lo, hi = GROUPS[g]

        @pl.when(own)
        def _():
            wait_cross(g)
            for slot in range(lo, hi):
                done[slot - NUM_LOCAL] = (part[slot, x] + cross[slot]).astype(BF16)

        for slot in range(lo, hi):
            p, h = FAR_SLOTS[slot - NUM_LOCAL]
            start(own & (x + 2 * h <= p - r), back_copies(slot - NUM_LOCAL))

    def finish_local():
        @pl.when(own)
        def _():
            wait_cross(0)
            below = lax.broadcasted_iota(jnp.int32, (BLK, BLK), 0) >= lax.broadcasted_iota(jnp.int32, (BLK, BLK), 1)
            for slot, (p, h) in enumerate(LOCAL_SLOTS):
                q = x + 2 * h

                @pl.when(q <= p)
                def _():
                    total = part[slot, x] + cross[slot]
                    keep = below | (q < p)
                    dl[rows(p), rows(h)] = jnp.where(keep, total, 0.0).astype(BF16)

    def far_outer(p, lo, num_q):
        def body(q, carry):
            part[lo + q // 2, q % 2] = outer(xr, p * BLK, q)
            return carry

        lax.fori_loop(0, num_q, body, 0)

    def row_sum(q, far_first, cols):
        near = lax.dot_general(wl[q, rows(q, 4 - q)], xl[rows(q, 4 - q), cols], (((0,), (0,)), ((), ())), preferred_element_type=F32)
        far = lax.dot_general(wr[q, rows(far_first, 4 - far_first)], xr[rows(far_first, 4 - far_first), cols], (((0,), (0,)), ((), ())), preferred_element_type=F32)
        return near + far

    def tile_loop(body):
        def step(j, carry):
            body(pl.ds(pl.multiple_of(j * TILE, TILE), TILE))
            return carry

        lax.fori_loop(0, num_cols // TILE, step, 0)

    def weights_here(q):
        h = q // 2
        arrived(wl.at[q] if h == 0 else wl.at[q, rows(2, 2)], wl_r.at[q])
        if h == 0:
            pl.when(other | (x != q))(lambda: arrived(near_dst(q, h), near_r.at[q]))
        else:
            pl.when(other | (x + 2 != q))(lambda: arrived(near_dst(q, h), near_r.at[q]))
        if q % 2 == 0:
            pl.when((r == 0) & jnp.logical_not(far_owner))(lambda: arrived(far_dst(q), far_r.at[h]))

    def block_row(q):
        weights_here(q)

        def body(cols):
            db[rows(q), cols] = row_sum(q, q, cols).astype(BF16)

        tile_loop(body)

    def chunk_copy(i, source):
        first, width = CHUNKS[i]
        cols = pl.ds(first, width)
        sems = bulk_s.at[3 + i], bulk_r.at[3 + i]
        return copy_to(across, source.at[rows(0), cols], xr.at[rows(0), cols], *sems)

    def start_chunks(span):
        for i in span:
            late_chunk = CHUNKS[i] in LATE
            start((r == 1) & (core == 0) if late_chunk else r == 1, chunk_copy(i, grad))
            if late_chunk:
                start(r == 0, chunk_copy(i, side))

    arrived(xr.at[rows(3)], bulk_r.at[0])
    push(0)
    far_outer(3, 6, 4)
    block_row(3)
    start(None, bulk(2, 1))
    for h in range(2):

        @pl.when(far_owner)
        def _():
            arrived(far_dst(2 * h), far_r.at[h])

        for n, device in enumerate((mate, next_chip, diagonal)):
            start(far_owner, copy_to(device, far_dst(2 * h), far_dst(2 * h), far_s.at[2 + 3 * h + n], far_r.at[h]))
    push(1)
    add_and_cross(0)
    add_and_cross(1)

    arrived(xr.at[rows(2)], bulk_r.at[1])
    finish_far(1)
    early = range(len(EARLY))
    late = range(len(EARLY), len(CHUNKS))
    start_chunks(early)
    far_outer(2, 8, 4)
    block_row(2)
    push(2)
    finish_local()
    add_and_cross(2)

    arrived(xr.at[rows(1)], bulk_r.at[2])
    start_chunks(late)
    finish_far(2)
    far_outer(1, 10, 2)
    block_row(1)
    push(3)
    weights_here(0)

    @pl.when(r == 0)
    def _():
        corner_weight[...] = wr[0, rows(0)]

    def first_row(cols):
        total = row_sum(0, 1, cols)

        @pl.when(r == 1)
        def _():
            db[rows(0), cols] = total.astype(BF16)

        @pl.when(r == 0)
        def _():
            acc[:, cols] = total

    def first_half(lo, hi):
        def step(j, carry):
            first_row(pl.ds(pl.multiple_of(j * TILE, TILE), TILE))
            return carry

        lax.fori_loop(lo, hi, step, 0)

    add_and_cross(3)
    first_half(0, num_cols // TILE)
    finish_far(3)

    corner[0] = jnp.zeros((BLK, BLK), F32)

    def nt_dot(left, right):
        return lax.dot_general(left, right, (((1,), (1,)), ((), ())), preferred_element_type=F32)

    def corner_in_row(row):
        start((r == row) & (core == 1), copy_to(mate, corner.at[0], corner.at[1], corner_s.at[0], corner_r.at[0]))
        owner = (r == row) & (core == 0)

        @pl.when(owner)
        def _():
            arrived(corner.at[1], corner_r.at[0])
            corner[0] += corner[1]

        start(owner & (x == 1), copy_to(next_chip, corner.at[0], corner.at[2], corner_s.at[1], corner_r.at[1]))

        @pl.when(owner & (x == 0))
        def _():
            arrived(corner.at[2], corner_r.at[1])

        return owner & (x == 0)

    for i, (first, width) in enumerate(CHUNKS):
        early_chunk = (first, width) in EARLY
        here = (r == 0) if early_chunk else (r == 1) | (core == 0)

        @pl.when(here)
        def _():
            arrived(xr.at[rows(0), pl.ds(first, width)], bulk_r.at[3 + i])

            def step(j, carry):
                cols = pl.ds(pl.multiple_of(first + j * TILE, TILE), TILE)

                @pl.when(r == 0)
                def _():
                    term = lax.dot_general(wr[0, rows(0)], xr[rows(0), cols], (((0,), (0,)), ((), ())), preferred_element_type=F32)
                    db[rows(0), cols] = (acc[:, cols] + term).astype(BF16)
                    if early_chunk:
                        corner[0] += nt_dot(xr[rows(0), cols], bl[rows(0), cols])

                if not early_chunk:

                    @pl.when(r == 1)
                    def _():
                        corner[0] += nt_dot(xl[rows(0), cols], xr[rows(0), cols])

                return carry

            lax.fori_loop(0, width // TILE, step, 0)

        if i == len(EARLY) - 1:
            first_device = corner_in_row(0)

            @pl.when(first_device)
            def _():
                corner[0] += corner[2]

            start(first_device, copy_to(across, corner.at[0], corner.at[3], corner_s.at[2], corner_r.at[2]))

    last_device = corner_in_row(1)

    @pl.when(last_device)
    def _():
        arrived(corner.at[3], corner_r.at[2])
        dl[rows(0), rows(0)] = (corner[0] + corner[2] + corner[3]).astype(BF16)

    for i, (p, h) in enumerate(FAR_SLOTS):
        pl.when(other & (x + 2 * h <= p + r - 1))(lambda: arrived(dl.at[rows(p), rows(h)], back_r.at[i]))
    for when, copy in sent:
        if when is None:
            copy.wait_send()
        else:
            pl.when(when)(copy.wait_send)


def per_device(lower, side, grad):
    num_rows, num_cols = grad.shape
    dma = pltpu.SemaphoreType.DMA
    num_bulk = 3 + len(CHUNKS)
    db, dl, acc, weight = pl.pallas_call(
        kernel,
        in_specs=[pl.BlockSpec(memory_space=pl.ANY)] * 3,
        out_specs=[pl.BlockSpec(memory_space=pltpu.VMEM)] * 4,
        out_shape=[pltpu.VMEM(grad.shape, BF16), pltpu.VMEM(lower.shape, BF16), pltpu.VMEM((BLK, num_cols), F32), pltpu.VMEM((BLK, BLK), BF16)],
        scratch_shapes=[
            pltpu.VMEM((num_rows, num_cols), BF16),
            pltpu.VMEM((num_rows, num_cols), BF16),
            pltpu.VMEM((num_rows, num_cols), BF16),
            pltpu.VMEM((4, 4 * BLK, BLK), BF16),
            pltpu.VMEM((4, 4 * BLK, BLK), BF16),
            pltpu.VMEM((2, BLK, BLK), BF16),
            pltpu.VMEM((NUM_SLOTS, 2, BLK, BLK), F32),
            pltpu.VMEM((NUM_SLOTS, 2, BLK, BLK), F32),
            pltpu.VMEM((NUM_SLOTS, BLK, BLK), F32),
            pltpu.VMEM((len(FAR_SLOTS), BLK, BLK), BF16),
            pltpu.VMEM((4, BLK, BLK), F32),
            dma((num_bulk,)), dma((num_bulk,)), dma((8,)), dma((6,)), dma((4,)), dma((8,)), dma((4,)), dma((8,)), dma((2,)), dma((2,)), dma((2,)),
            dma((4,)), dma((4,)), dma((4,)), dma((4,)), dma((5,)), dma((5,)), dma((3,)), dma((3,)),
        ],
        compiler_params=pltpu.CompilerParams(collective_id=0, has_side_effects=True, vmem_limit_bytes=49 * 1024 * 1024),
    )(lower, side, grad)
    in_vmem = pl.BlockSpec(memory_space=pltpu.VMEM)
    anywhere = pl.BlockSpec(memory_space=pl.ANY)

    def keep(value):
        return pltpu.with_memory_space_constraint(value, pltpu.VMEM)

    in_hbm = pl.BlockSpec(memory_space=pltpu.HBM)

    def stay(value):
        return pltpu.with_memory_space_constraint(value, pltpu.HBM)

    db, dl = pl.pallas_call(
        put_kernel,
        in_specs=[in_vmem] * 2,
        out_specs=[anywhere] * 2,
        out_shape=[jax.ShapeDtypeStruct(grad.shape, BF16), jax.ShapeDtypeStruct(lower.shape, BF16)],
        scratch_shapes=[dma((5,))],
        compiler_params=pltpu.CompilerParams(vmem_limit_bytes=1024 * 1024),
    )(keep(db), keep(dl))
    width = sum(w for _, w in LATE)
    tail = pl.pallas_call(
        tail_kernel,
        in_specs=[in_hbm, in_vmem, in_vmem, in_hbm],
        out_specs=in_vmem,
        out_shape=pltpu.VMEM((BLK, width), BF16),
        scratch_shapes=[pltpu.VMEM((BLK, width), BF16), dma((len(LATE),)), dma((len(LATE),))],
        compiler_params=pltpu.CompilerParams(collective_id=1, has_side_effects=True, vmem_limit_bytes=4 * 1024 * 1024),
    )(stay(grad), keep(acc), keep(weight), stay(dl))
    db = pl.pallas_call(
        put_tail_kernel,
        in_specs=[anywhere, in_vmem],
        out_specs=anywhere,
        out_shape=jax.ShapeDtypeStruct(grad.shape, BF16),
        input_output_aliases={0: 0},
        scratch_shapes=[dma],
        compiler_params=pltpu.CompilerParams(vmem_limit_bytes=1024 * 1024),
    )(db, keep(tail))
    return db, dl


def put_kernel(db_in, dl_in, db_out, dl_out, sems):
    copies = [pltpu.make_async_copy(dl_in, dl_out, sems.at[0])]
    copies += [pltpu.make_async_copy(db_in.at[rows(i)], db_out.at[rows(i)], sems.at[1 + i]) for i in range(4)]
    for copy in copies:
        copy.start()
    for copy in copies:
        copy.wait()


def tail_kernel(grad, acc, weight, dl, tail, arriving, send_sem, recv_sem):
    del dl
    r = lax.axis_index("row")
    core = lax.axis_index("col") % 2
    sender = (r == 1) & (core == 1)
    receiver = (r == 0) & (core == 1)
    barrier = pltpu.get_barrier_semaphore()
    pl.when(receiver)(lambda: pl.semaphore_signal(barrier, inc=1, device_id={"row": 1 - r}, device_id_type=MESH))
    pl.when(sender)(lambda: pl.semaphore_wait(barrier, 1))
    base = LATE[0][0]
    copies = []
    for i, (first, width) in enumerate(LATE):
        copies.append(pltpu.make_async_remote_copy(
            src_ref=grad.at[rows(0), pl.ds(first, width)], dst_ref=arriving.at[:, pl.ds(first - base, width)],
            send_sem=send_sem.at[i], recv_sem=recv_sem.at[i], device_id={"row": 1 - r}, device_id_type=MESH))
        pl.when(sender)(copies[i].start)
    for i, (first, width) in enumerate(LATE):

        @pl.when(receiver)
        def _():
            copies[i].wait_recv()
            for n in range(width // TILE):
                at = first - base + n * TILE
                term = lax.dot_general(weight[...], arriving[:, pl.ds(at, TILE)], (((0,), (0,)), ((), ())), preferred_element_type=F32)
                tail[:, pl.ds(at, TILE)] = (acc[:, pl.ds(base + at, TILE)] + term).astype(BF16)

        pl.when(sender)(copies[i].wait_send)


def put_tail_kernel(db_in, tail, db_out, sem):
    del db_in

    @pl.when((lax.axis_index("row") == 0) & (lax.axis_index("col") % 2 == 1))
    def _():
        copy = pltpu.make_async_copy(tail, db_out.at[rows(0), pl.ds(LATE[0][0], tail.shape[1])], sem)
        copy.start()
        copy.wait()


def solution(mesh):
    spec = P(("batch", "row"), "col")
    return jax.shard_map(per_device, mesh=mesh, in_specs=(spec, spec, spec), out_specs=(spec, spec), check_vma=False)
```

```python
import jax
import jax.numpy as jnp
from jax import lax
from jax.experimental import pallas as pl
from jax.experimental.pallas import tpu as pltpu
from jax.sharding import PartitionSpec as P

BLK = 256
F32 = jnp.float32
BF16 = jnp.bfloat16
MESH = pl.DeviceIdType.MESH
TILE = 256
EARLY = ((0, 2304),)
LATE = ((2304, 1536), (3840, 256),)
CHUNKS = EARLY + LATE
LOCAL_SLOTS = ((0, 0), (1, 0), (2, 0), (3, 0), (2, 1), (3, 1))
FAR_SLOTS = ((3, 0), (3, 1), (2, 0), (2, 1), (1, 0))
NUM_LOCAL = len(LOCAL_SLOTS)
NUM_SLOTS = NUM_LOCAL + len(FAR_SLOTS)
GROUPS = ((0, 6), (6, 8), (8, 10), (10, 11))


def rows(p, n=1):
    return pl.ds(p * BLK, n * BLK)


def kernel(lower, side, grad, db, dl, acc, corner_weight, xr, xl, bl, wl, wr, relay, part, peer, cross, done, corner,
           bulk_s, bulk_r, load_s, wl_s, wl_r, near_s, near_r, far_s, far_r, relay_s, relay_r, push_s, push_r, cross_s, cross_r, back_s, back_r, corner_s, corner_r):
    r = lax.axis_index("row")
    c = lax.axis_index("col")
    x = c // 2
    core = c % 2
    own = core == r
    other = core != r
    across = {"row": 1 - r}
    mate = {"col": 2 * x + 1 - core}
    next_chip = {"col": 2 * (1 - x) + core}
    diagonal = {"col": 2 * (1 - x) + 1 - core}
    num_cols = grad.shape[1]
    sent = []

    def copy_to(device, src, dst, send_sem, recv_sem):
        return pltpu.make_async_remote_copy(src_ref=src, dst_ref=dst, send_sem=send_sem, recv_sem=recv_sem, device_id=device, device_id_type=MESH)

    def start(when, copy):
        sent.append((when, copy))
        if when is None:
            copy.start()
        else:
            pl.when(when)(copy.start)

    def arrived(ref, sem):
        pltpu.make_async_copy(ref, ref, sem).wait()

    barrier = pltpu.get_barrier_semaphore()

    def greet(when, *devices):
        @pl.when(when)
        def _():
            for device in devices:
                pl.semaphore_signal(barrier, inc=1, device_id=device, device_id_type=MESH)

    first_core = core == 1
    second_core = core == 0
    greet(first_core, across)
    greet(second_core, across, next_chip)
    pl.when(first_core)(lambda: pl.semaphore_wait(barrier, 1))

    near_src = (lower.at[pl.ds(BLK, 3 * BLK), pl.ds(0, BLK)], lower.at[pl.ds(3 * BLK, BLK), pl.ds(BLK, BLK)])
    far_src = (lower.at[pl.ds(0, BLK), pl.ds(0, BLK)], lower.at[pl.ds(2 * BLK, BLK), pl.ds(BLK, BLK)])

    def near_dst(q, h):
        return wr.at[q, rows(1, 3)] if h == 0 else wr.at[q, rows(3)]

    def far_dst(q):
        return wr.at[q, rows(q)]

    def bulk(i, p):
        return copy_to(across, grad.at[rows(p)], xr.at[rows(p)], bulk_s.at[i], bulk_r.at[i])

    def first_copies(when):
        for h in range(2):
            start(when & other, copy_to(across, near_src[h], near_dst(x + 2 * h, h), near_s.at[h], near_r.at[x + 2 * h]))
        start(when, bulk(0, 3))

    first_copies(first_core)
    greet(first_core, mate, diagonal)
    pl.when(second_core)(lambda: pl.semaphore_wait(barrier, 4))
    first_copies(second_core)
    greet(second_core, mate)
    pl.when(first_core)(lambda: pl.semaphore_wait(barrier, 1))

    far_sender = other & (r == 1) & (x == 0)
    for h in range(2):
        start(far_sender, copy_to(diagonal, far_src[h], relay.at[h], far_s.at[h], relay_r.at[h]))

    loads = [pltpu.make_async_copy(side.at[rows(q)], bl.at[rows(q)], load_s.at[q]) for q in range(4)]
    loads += [pltpu.make_async_copy(grad.at[rows(p)], xl.at[rows(p)], load_s.at[4 + p]) for p in range(4)]
    for load in loads:
        load.start()

    for h in range(2):
        src = lower.at[:, pl.ds(0, BLK)] if h == 0 else lower.at[rows(2, 2), pl.ds(BLK, BLK)]
        q = x + 2 * h
        dst = wl.at[q] if h == 0 else wl.at[q, rows(2, 2)]
        pl.when(own)(pltpu.make_async_copy(src, dst, wl_r.at[q]).start)
        for n, device in enumerate((mate, next_chip, diagonal)):
            start(own, copy_to(device, src, dst, wl_s.at[3 * h + n], wl_r.at[q]))

    @pl.when(r == 1)
    def _():
        wr[2, rows(2)] = jnp.zeros((BLK, BLK), BF16)

    for p in range(4):
        for h in range(2):
            far_zero = (x + 2 * h > p + r - 1) if p else (x >= 0)
            zero = (other & far_zero) | (own & (x + 2 * h > p))

            @pl.when(zero)
            def _():
                dl[rows(p), rows(h)] = jnp.zeros((BLK, BLK), BF16)

    def outer(left, left_row, q):
        total = None
        for k in range(0, num_cols, 1024):
            term = lax.dot_general(left[pl.ds(left_row, BLK), pl.ds(k, 1024)], bl[pl.ds(q * BLK, BLK), pl.ds(k, 1024)], (((1,), (1,)), ((), ())), preferred_element_type=F32)
            total = term if total is None else total + term
        return total

    for load in loads:
        load.wait()

    def local_outer(i, carry):
        slot, parity = i // 2, i % 2
        h = slot // 4
        p = slot - 2 * h
        part[slot, parity] = outer(xl, pl.multiple_of(p * BLK, BLK), 2 * h + parity)
        return carry

    lax.fori_loop(0, 2 * NUM_LOCAL, local_outer, 0)

    for h in range(2):
        q = x + 2 * h

        @pl.when(own)
        def _():
            arrived(near_dst(q, h), near_r.at[q])

        for n, device in enumerate((mate, next_chip, diagonal)):
            start(own, copy_to(device, near_dst(q, h), near_dst(q, h), near_s.at[2 + 3 * h + n], near_r.at[q]))
    far_owner = other & (r == 0) & (x == 1)
    relay_here = own & (r == 1) & (x == 1)
    for h in range(2):

        @pl.when(relay_here)
        def _():
            arrived(relay.at[h], relay_r.at[h])

        start(relay_here, copy_to(across, relay.at[h], far_dst(2 * h), relay_s.at[h], far_r.at[h]))
    start(None, bulk(1, 2))

    def push(g):
        lo, hi = GROUPS[g]
        span = pl.ds(lo, hi - lo)
        start(other, copy_to(mate, part.at[span], peer.at[span], push_s.at[g], push_r.at[g]))

    def add_and_cross(g):
        lo, hi = GROUPS[g]
        span = pl.ds(lo, hi - lo)

        @pl.when(own)
        def _():
            arrived(peer.at[span], push_r.at[g])

            def add(slot, carry):
                part[slot] = part[slot] + peer[slot]
                return carry

            lax.fori_loop(lo, hi, add, 0)

        start(own, copy_to(next_chip, part.at[span, 1 - x], cross.at[span], cross_s.at[g], cross_r.at[g]))

    def wait_cross(g):
        lo, hi = GROUPS[g]
        arrived(cross.at[pl.ds(lo, hi - lo)], cross_r.at[g])

    def back_copies(i):
        p, h = FAR_SLOTS[i]
        return copy_to(across, done.at[i], dl.at[rows(p), rows(h)], back_s.at[i], back_r.at[i])

    def finish_far(g):
        lo, hi = GROUPS[g]

        @pl.when(own)
        def _():
            wait_cross(g)
            for slot in range(lo, hi):
                done[slot - NUM_LOCAL] = (part[slot, x] + cross[slot]).astype(BF16)

        for slot in range(lo, hi):
            p, h = FAR_SLOTS[slot - NUM_LOCAL]
            start(own & (x + 2 * h <= p - r), back_copies(slot - NUM_LOCAL))

    def finish_local():
        @pl.when(own)
        def _():
            wait_cross(0)
            below = lax.broadcasted_iota(jnp.int32, (BLK, BLK), 0) >= lax.broadcasted_iota(jnp.int32, (BLK, BLK), 1)
            for slot, (p, h) in enumerate(LOCAL_SLOTS):
                q = x + 2 * h

                @pl.when(q <= p)
                def _():
                    total = part[slot, x] + cross[slot]
                    keep = below | (q < p)
                    dl[rows(p), rows(h)] = jnp.where(keep, total, 0.0).astype(BF16)

    def far_outer(p, lo, num_q):
        def body(q, carry):
            part[lo + q // 2, q % 2] = outer(xr, p * BLK, q)
            return carry

        lax.fori_loop(0, num_q, body, 0)

    def row_sum(q, far_first, cols):
        near = lax.dot_general(wl[q, rows(q, 4 - q)], xl[rows(q, 4 - q), cols], (((0,), (0,)), ((), ())), preferred_element_type=F32)
        far = lax.dot_general(wr[q, rows(far_first, 4 - far_first)], xr[rows(far_first, 4 - far_first), cols], (((0,), (0,)), ((), ())), preferred_element_type=F32)
        return near + far

    def tile_loop(body):
        def step(j, carry):
            body(pl.ds(pl.multiple_of(j * TILE, TILE), TILE))
            return carry

        lax.fori_loop(0, num_cols // TILE, step, 0)

    def weights_here(q):
        h = q // 2
        arrived(wl.at[q] if h == 0 else wl.at[q, rows(2, 2)], wl_r.at[q])
        if h == 0:
            pl.when(other | (x != q))(lambda: arrived(near_dst(q, h), near_r.at[q]))
        else:
            pl.when(other | (x + 2 != q))(lambda: arrived(near_dst(q, h), near_r.at[q]))
        if q % 2 == 0:
            pl.when((r == 0) & jnp.logical_not(far_owner))(lambda: arrived(far_dst(q), far_r.at[h]))

    def block_row(q):
        weights_here(q)

        def body(cols):
            db[rows(q), cols] = row_sum(q, q, cols).astype(BF16)

        tile_loop(body)

    def chunk_copy(i, source):
        first, width = CHUNKS[i]
        cols = pl.ds(first, width)
        sems = bulk_s.at[3 + i], bulk_r.at[3 + i]
        return copy_to(across, source.at[rows(0), cols], xr.at[rows(0), cols], *sems)

    def start_chunks(span):
        for i in span:
            late_chunk = CHUNKS[i] in LATE
            start((r == 1) & (core == 0) if late_chunk else r == 1, chunk_copy(i, grad))
            if late_chunk:
                start(r == 0, chunk_copy(i, side))

    arrived(xr.at[rows(3)], bulk_r.at[0])
    push(0)
    far_outer(3, 6, 4)
    block_row(3)
    start(None, bulk(2, 1))
    for h in range(2):

        @pl.when(far_owner)
        def _():
            arrived(far_dst(2 * h), far_r.at[h])

        for n, device in enumerate((mate, next_chip, diagonal)):
            start(far_owner, copy_to(device, far_dst(2 * h), far_dst(2 * h), far_s.at[2 + 3 * h + n], far_r.at[h]))
    push(1)
    add_and_cross(0)
    add_and_cross(1)

    arrived(xr.at[rows(2)], bulk_r.at[1])
    finish_far(1)
    early = range(len(EARLY))
    late = range(len(EARLY), len(CHUNKS))
    start_chunks(early)
    far_outer(2, 8, 4)
    block_row(2)
    push(2)
    finish_local()
    add_and_cross(2)

    arrived(xr.at[rows(1)], bulk_r.at[2])
    start_chunks(late)
    finish_far(2)
    far_outer(1, 10, 2)
    block_row(1)
    push(3)
    weights_here(0)

    @pl.when(r == 0)
    def _():
        corner_weight[...] = wr[0, rows(0)]

    def first_row(cols):
        total = row_sum(0, 1, cols)

        @pl.when(r == 1)
        def _():
            db[rows(0), cols] = total.astype(BF16)

        @pl.when(r == 0)
        def _():
            acc[:, cols] = total

    def first_half(lo, hi):
        def step(j, carry):
            first_row(pl.ds(pl.multiple_of(j * TILE, TILE), TILE))
            return carry

        lax.fori_loop(lo, hi, step, 0)

    add_and_cross(3)
    first_half(0, num_cols // TILE)
    finish_far(3)

    corner[0] = jnp.zeros((BLK, BLK), F32)

    def nt_dot(left, right):
        return lax.dot_general(left, right, (((1,), (1,)), ((), ())), preferred_element_type=F32)

    def corner_in_row(row):
        start((r == row) & (core == 1), copy_to(mate, corner.at[0], corner.at[1], corner_s.at[0], corner_r.at[0]))
        owner = (r == row) & (core == 0)

        @pl.when(owner)
        def _():
            arrived(corner.at[1], corner_r.at[0])
            corner[0] += corner[1]

        start(owner & (x == 1), copy_to(next_chip, corner.at[0], corner.at[2], corner_s.at[1], corner_r.at[1]))

        @pl.when(owner & (x == 0))
        def _():
            arrived(corner.at[2], corner_r.at[1])

        return owner & (x == 0)

    for i, (first, width) in enumerate(CHUNKS):
        early_chunk = (first, width) in EARLY
        here = (r == 0) if early_chunk else (r == 1) | (core == 0)

        @pl.when(here)
        def _():
            arrived(xr.at[rows(0), pl.ds(first, width)], bulk_r.at[3 + i])

            def step(j, carry):
                cols = pl.ds(pl.multiple_of(first + j * TILE, TILE), TILE)

                @pl.when(r == 0)
                def _():
                    term = lax.dot_general(wr[0, rows(0)], xr[rows(0), cols], (((0,), (0,)), ((), ())), preferred_element_type=F32)
                    db[rows(0), cols] = (acc[:, cols] + term).astype(BF16)
                    if early_chunk:
                        corner[0] += nt_dot(xr[rows(0), cols], bl[rows(0), cols])

                if not early_chunk:

                    @pl.when(r == 1)
                    def _():
                        corner[0] += nt_dot(xl[rows(0), cols], xr[rows(0), cols])

                return carry

            lax.fori_loop(0, width // TILE, step, 0)

        if i == len(EARLY) - 1:
            first_device = corner_in_row(0)

            @pl.when(first_device)
            def _():
                corner[0] += corner[2]

            start(first_device, copy_to(across, corner.at[0], corner.at[3], corner_s.at[2], corner_r.at[2]))

    last_device = corner_in_row(1)

    @pl.when(last_device)
    def _():
        arrived(corner.at[3], corner_r.at[2])
        dl[rows(0), rows(0)] = (corner[0] + corner[2] + corner[3]).astype(BF16)

    for i, (p, h) in enumerate(FAR_SLOTS):
        pl.when(other & (x + 2 * h <= p + r - 1))(lambda: arrived(dl.at[rows(p), rows(h)], back_r.at[i]))
    for when, copy in sent:
        if when is None:
            copy.wait_send()
        else:
            pl.when(when)(copy.wait_send)


def per_device(lower, side, grad):
    num_rows, num_cols = grad.shape
    dma = pltpu.SemaphoreType.DMA
    num_bulk = 3 + len(CHUNKS)
    db, dl, acc, weight = pl.pallas_call(
        kernel,
        in_specs=[pl.BlockSpec(memory_space=pl.ANY)] * 3,
        out_specs=[pl.BlockSpec(memory_space=pltpu.VMEM)] * 4,
        out_shape=[pltpu.VMEM(grad.shape, BF16), pltpu.VMEM(lower.shape, BF16), pltpu.VMEM((BLK, num_cols), F32), pltpu.VMEM((BLK, BLK), BF16)],
        scratch_shapes=[
            pltpu.VMEM((num_rows, num_cols), BF16),
            pltpu.VMEM((num_rows, num_cols), BF16),
            pltpu.VMEM((num_rows, num_cols), BF16),
            pltpu.VMEM((4, 4 * BLK, BLK), BF16),
            pltpu.VMEM((4, 4 * BLK, BLK), BF16),
            pltpu.VMEM((2, BLK, BLK), BF16),
            pltpu.VMEM((NUM_SLOTS, 2, BLK, BLK), F32),
            pltpu.VMEM((NUM_SLOTS, 2, BLK, BLK), F32),
            pltpu.VMEM((NUM_SLOTS, BLK, BLK), F32),
            pltpu.VMEM((len(FAR_SLOTS), BLK, BLK), BF16),
            pltpu.VMEM((4, BLK, BLK), F32),
            dma((num_bulk,)), dma((num_bulk,)), dma((8,)), dma((6,)), dma((4,)), dma((8,)), dma((4,)), dma((8,)), dma((2,)), dma((2,)), dma((2,)),
            dma((4,)), dma((4,)), dma((4,)), dma((4,)), dma((5,)), dma((5,)), dma((3,)), dma((3,)),
        ],
        compiler_params=pltpu.CompilerParams(collective_id=0, has_side_effects=True, vmem_limit_bytes=49 * 1024 * 1024),
    )(lower, side, grad)
    in_vmem = pl.BlockSpec(memory_space=pltpu.VMEM)
    anywhere = pl.BlockSpec(memory_space=pl.ANY)

    def keep(value):
        return pltpu.with_memory_space_constraint(value, pltpu.VMEM)

    in_hbm = pl.BlockSpec(memory_space=pltpu.HBM)

    def stay(value):
        return pltpu.with_memory_space_constraint(value, pltpu.HBM)

    db, dl = pl.pallas_call(
        put_kernel,
        in_specs=[in_vmem] * 2,
        out_specs=[anywhere] * 2,
        out_shape=[jax.ShapeDtypeStruct(grad.shape, BF16), jax.ShapeDtypeStruct(lower.shape, BF16)],
        scratch_shapes=[dma((5,))],
        compiler_params=pltpu.CompilerParams(vmem_limit_bytes=1024 * 1024),
    )(keep(db), keep(dl))
    width = sum(w for _, w in LATE)
    tail = pl.pallas_call(
        tail_kernel,
        in_specs=[in_hbm, in_vmem, in_vmem, in_hbm],
        out_specs=in_vmem,
        out_shape=pltpu.VMEM((BLK, width), BF16),
        scratch_shapes=[pltpu.VMEM((BLK, width), BF16), dma((len(LATE),)), dma((len(LATE),))],
        compiler_params=pltpu.CompilerParams(collective_id=1, has_side_effects=True, vmem_limit_bytes=4 * 1024 * 1024),
    )(stay(grad), keep(acc), keep(weight), stay(dl))
    db = pl.pallas_call(
        put_tail_kernel,
        in_specs=[anywhere, in_vmem],
        out_specs=anywhere,
        out_shape=jax.ShapeDtypeStruct(grad.shape, BF16),
        input_output_aliases={0: 0},
        scratch_shapes=[dma],
        compiler_params=pltpu.CompilerParams(vmem_limit_bytes=1024 * 1024),
    )(db, keep(tail))
    return db, dl


def put_kernel(db_in, dl_in, db_out, dl_out, sems):
    copies = [pltpu.make_async_copy(dl_in, dl_out, sems.at[0])]
    copies += [pltpu.make_async_copy(db_in.at[rows(i)], db_out.at[rows(i)], sems.at[1 + i]) for i in range(4)]
    for copy in copies:
        copy.start()
    for copy in copies:
        copy.wait()


def tail_kernel(grad, acc, weight, dl, tail, arriving, send_sem, recv_sem):
    del dl
    r = lax.axis_index("row")
    core = lax.axis_index("col") % 2
    sender = (r == 1) & (core == 1)
    receiver = (r == 0) & (core == 1)
    barrier = pltpu.get_barrier_semaphore()
    pl.when(receiver)(lambda: pl.semaphore_signal(barrier, inc=1, device_id={"row": 1 - r}, device_id_type=MESH))
    pl.when(sender)(lambda: pl.semaphore_wait(barrier, 1))
    base = LATE[0][0]
    copies = []
    for i, (first, width) in enumerate(LATE):
        copies.append(pltpu.make_async_remote_copy(
            src_ref=grad.at[rows(0), pl.ds(first, width)], dst_ref=arriving.at[:, pl.ds(first - base, width)],
            send_sem=send_sem.at[i], recv_sem=recv_sem.at[i], device_id={"row": 1 - r}, device_id_type=MESH))
        pl.when(sender)(copies[i].start)
    for i, (first, width) in enumerate(LATE):

        @pl.when(receiver)
        def _():
            copies[i].wait_recv()
            for n in range(width // TILE):
                at = first - base + n * TILE
                term = lax.dot_general(weight[...], arriving[:, pl.ds(at, TILE)], (((0,), (0,)), ((), ())), preferred_element_type=F32)
                tail[:, pl.ds(at, TILE)] = (acc[:, pl.ds(base + at, TILE)] + term).astype(BF16)

        pl.when(sender)(copies[i].wait_send)


def put_tail_kernel(db_in, tail, db_out, sem):
    del db_in

    @pl.when((lax.axis_index("row") == 0) & (lax.axis_index("col") % 2 == 1))
    def _():
        copy = pltpu.make_async_copy(tail, db_out.at[rows(0), pl.ds(LATE[0][0], tail.shape[1])], sem)
        copy.start()
        copy.wait()


def solution(mesh):
    spec = P(("batch", "row"), "col")
    return jax.shard_map(per_device, mesh=mesh, in_specs=(spec, spec, spec), out_specs=(spec, spec), check_vma=False)
```

```python
import jax
import jax.numpy as jnp
from jax import lax
from jax.experimental import pallas as pl
from jax.experimental.pallas import tpu as pltpu
from jax.sharding import PartitionSpec as P

BLK = 256
F32 = jnp.float32
BF16 = jnp.bfloat16
MESH = pl.DeviceIdType.MESH
TILE = 256
SHIFT = 64
EARLY = ((0, 2304),)
LATE = ((2304, 1536), (3840, 256),)
CHUNKS = EARLY + LATE
LOCAL_SLOTS = ((0, 0), (1, 0), (2, 0), (3, 0), (2, 1), (3, 1))
FAR_SLOTS = ((3, 0), (3, 1), (2, 0), (2, 1), (1, 0))
NUM_LOCAL = len(LOCAL_SLOTS)
NUM_SLOTS = NUM_LOCAL + len(FAR_SLOTS)
GROUPS = ((0, 6), (6, 8), (8, 10), (10, 11))


def rows(p, n=1):
    return pl.ds(p * BLK, n * BLK)


def kernel(lower, side, grad, db, dl, acc, corner_weight, xr, xl, bl, wl, wr, relay, part, peer, cross, done, corner,
           bulk_s, bulk_r, load_s, wl_s, wl_r, near_s, near_r, far_s, far_r, relay_s, relay_r, push_s, push_r, cross_s, cross_r, back_s, back_r, corner_s, corner_r):
    r = lax.axis_index("row")
    c = lax.axis_index("col")
    x = c // 2
    core = c % 2
    own = core == r
    other = core != r
    across = {"row": 1 - r}
    mate = {"col": 2 * x + 1 - core}
    next_chip = {"col": 2 * (1 - x) + core}
    diagonal = {"col": 2 * (1 - x) + 1 - core}
    num_cols = grad.shape[1]
    sent = []

    def copy_to(device, src, dst, send_sem, recv_sem):
        return pltpu.make_async_remote_copy(src_ref=src, dst_ref=dst, send_sem=send_sem, recv_sem=recv_sem, device_id=device, device_id_type=MESH)

    def start(when, copy):
        sent.append((when, copy))
        if when is None:
            copy.start()
        else:
            pl.when(when)(copy.start)

    def arrived(ref, sem):
        pltpu.make_async_copy(ref, ref, sem).wait()

    barrier = pltpu.get_barrier_semaphore()

    def greet(when, *devices):
        @pl.when(when)
        def _():
            for device in devices:
                pl.semaphore_signal(barrier, inc=1, device_id=device, device_id_type=MESH)

    first_core = core == 1
    second_core = core == 0
    greet(first_core, across)
    greet(second_core, across, next_chip)
    pl.when(first_core)(lambda: pl.semaphore_wait(barrier, 1))

    def low_rows(short):
        return pl.ds(3 * BLK + SHIFT, BLK - SHIFT) if short else rows(3)

    def near_src(h, short):
        return lower.at[rows(1, 3), pl.ds(0, BLK)] if h == 0 else lower.at[low_rows(short), pl.ds(BLK, BLK)]

    def near_dst(q, h, short=False):
        return wr.at[q, rows(1, 3)] if h == 0 else wr.at[q, low_rows(short)]

    far_rows = (rows(0), pl.ds(2 * BLK, BLK + SHIFT))
    far_src = tuple(lower.at[far_rows[h], pl.ds(h * BLK, BLK)] for h in range(2))
    far_via = (relay.at[0, pl.ds(0, BLK)], relay.at[1])

    def far_dst(h):
        return wr.at[2 * h, far_rows[h]]

    far_sender = other & (r == 1) & (x == 0)
    near_kinds = ((0, False, other, r >= 0), (1, False, other & jnp.logical_not(far_sender), (r == 1) | (x == 1)), (1, True, far_sender, (r == 0) & (x == 0)))

    def bulk(i, p):
        return copy_to(across, grad.at[rows(p)], xr.at[rows(p)], bulk_s.at[i], bulk_r.at[i])

    def first_copies(when):
        for h, short, sends, _ in near_kinds:
            start(when & sends, copy_to(across, near_src(h, short), near_dst(x + 2 * h, h, short), near_s.at[h], near_r.at[x + 2 * h]))
        start(when, bulk(0, 3))

    first_copies(first_core)
    greet(first_core, mate, diagonal)
    pl.when(second_core)(lambda: pl.semaphore_wait(barrier, 4))
    first_copies(second_core)
    greet(second_core, mate)
    pl.when(first_core)(lambda: pl.semaphore_wait(barrier, 1))

    for h in range(2):
        start(far_sender, copy_to(diagonal, far_src[h], far_via[h], far_s.at[h], relay_r.at[h]))

    loads = [pltpu.make_async_copy(side.at[rows(q)], bl.at[rows(q)], load_s.at[q]) for q in range(4)]
    loads += [pltpu.make_async_copy(grad.at[rows(p)], xl.at[rows(p)], load_s.at[4 + p]) for p in range(4)]
    for load in loads:
        load.start()

    for h in range(2):
        src = lower.at[:, pl.ds(0, BLK)] if h == 0 else lower.at[rows(2, 2), pl.ds(BLK, BLK)]
        q = x + 2 * h
        dst = wl.at[q] if h == 0 else wl.at[q, rows(2, 2)]
        pl.when(own)(pltpu.make_async_copy(src, dst, wl_r.at[q]).start)
        for n, device in enumerate((mate, next_chip, diagonal)):
            start(own, copy_to(device, src, dst, wl_s.at[3 * h + n], wl_r.at[q]))

    @pl.when(r == 1)
    def _():
        wr[2, rows(2)] = jnp.zeros((BLK, BLK), BF16)

    for p in range(4):
        for h in range(2):
            far_zero = (x + 2 * h > p + r - 1) if p else (x >= 0)
            zero = (other & far_zero) | (own & (x + 2 * h > p))

            @pl.when(zero)
            def _():
                dl[rows(p), rows(h)] = jnp.zeros((BLK, BLK), BF16)

    def outer(left, left_row, q):
        total = None
        for k in range(0, num_cols, 1024):
            term = lax.dot_general(left[pl.ds(left_row, BLK), pl.ds(k, 1024)], bl[pl.ds(q * BLK, BLK), pl.ds(k, 1024)], (((1,), (1,)), ((), ())), preferred_element_type=F32)
            total = term if total is None else total + term
        return total

    for load in loads:
        load.wait()

    def local_outer(i, carry):
        slot, parity = i // 2, i % 2
        h = slot // 4
        p = slot - 2 * h
        part[slot, parity] = outer(xl, pl.multiple_of(p * BLK, BLK), 2 * h + parity)
        return carry

    lax.fori_loop(0, 2 * NUM_LOCAL, local_outer, 0)

    for h, short, _, receives in near_kinds:
        q = x + 2 * h
        there = near_dst(q, h, short)
        pl.when(own & receives)(lambda: arrived(there, near_r.at[q]))
        for n, device in enumerate((mate, next_chip, diagonal)):
            start(own & receives, copy_to(device, there, there, near_s.at[2 + 3 * h + n], near_r.at[q]))
    far_owner = other & (r == 0) & (x == 1)
    relay_here = own & (r == 1) & (x == 1)
    for h in range(2):

        @pl.when(relay_here)
        def _():
            arrived(far_via[h], relay_r.at[h])

        start(relay_here, copy_to(across, far_via[h], far_dst(h), relay_s.at[h], far_r.at[h]))
    start(None, bulk(1, 2))

    def push(g):
        lo, hi = GROUPS[g]
        span = pl.ds(lo, hi - lo)
        start(other, copy_to(mate, part.at[span], peer.at[span], push_s.at[g], push_r.at[g]))

    def add_and_cross(g):
        lo, hi = GROUPS[g]
        span = pl.ds(lo, hi - lo)

        @pl.when(own)
        def _():
            arrived(peer.at[span], push_r.at[g])

            def add(slot, carry):
                part[slot] = part[slot] + peer[slot]
                return carry

            lax.fori_loop(lo, hi, add, 0)

        start(own, copy_to(next_chip, part.at[span, 1 - x], cross.at[span], cross_s.at[g], cross_r.at[g]))

    def wait_cross(g):
        lo, hi = GROUPS[g]
        arrived(cross.at[pl.ds(lo, hi - lo)], cross_r.at[g])

    def back_copies(i):
        p, h = FAR_SLOTS[i]
        return copy_to(across, done.at[i], dl.at[rows(p), rows(h)], back_s.at[i], back_r.at[i])

    def finish_far(g):
        lo, hi = GROUPS[g]

        @pl.when(own)
        def _():
            wait_cross(g)
            for slot in range(lo, hi):
                done[slot - NUM_LOCAL] = (part[slot, x] + cross[slot]).astype(BF16)

        for slot in range(lo, hi):
            p, h = FAR_SLOTS[slot - NUM_LOCAL]
            start(own & (x + 2 * h <= p - r), back_copies(slot - NUM_LOCAL))

    def finish_local():
        @pl.when(own)
        def _():
            wait_cross(0)
            below = lax.broadcasted_iota(jnp.int32, (BLK, BLK), 0) >= lax.broadcasted_iota(jnp.int32, (BLK, BLK), 1)
            for slot, (p, h) in enumerate(LOCAL_SLOTS):
                q = x + 2 * h

                @pl.when(q <= p)
                def _():
                    total = part[slot, x] + cross[slot]
                    keep = below | (q < p)
                    dl[rows(p), rows(h)] = jnp.where(keep, total, 0.0).astype(BF16)

    def far_outer(p, lo, num_q):
        def body(q, carry):
            part[lo + q // 2, q % 2] = outer(xr, p * BLK, q)
            return carry

        lax.fori_loop(0, num_q, body, 0)

    def row_sum(q, far_first, cols):
        near = lax.dot_general(wl[q, rows(q, 4 - q)], xl[rows(q, 4 - q), cols], (((0,), (0,)), ((), ())), preferred_element_type=F32)
        far = lax.dot_general(wr[q, rows(far_first, 4 - far_first)], xr[rows(far_first, 4 - far_first), cols], (((0,), (0,)), ((), ())), preferred_element_type=F32)
        return near + far

    def tile_loop(body):
        def step(j, carry):
            body(pl.ds(pl.multiple_of(j * TILE, TILE), TILE))
            return carry

        lax.fori_loop(0, num_cols // TILE, step, 0)

    def weights_here(q):
        h = q // 2
        arrived(wl.at[q] if h == 0 else wl.at[q, rows(2, 2)], wl_r.at[q])
        elsewhere = other | (x + 2 * h != q)
        if q == 2:
            pl.when(elsewhere & (r == 0))(lambda: arrived(near_dst(q, h, True), near_r.at[q]))
            pl.when(elsewhere & (r == 1))(lambda: arrived(near_dst(q, h), near_r.at[q]))
        else:
            pl.when(elsewhere)(lambda: arrived(near_dst(q, h), near_r.at[q]))
        if q % 2 == 0:
            pl.when((r == 0) & jnp.logical_not(far_owner))(lambda: arrived(far_dst(h), far_r.at[h]))

    def block_row(q):
        weights_here(q)

        def body(cols):
            db[rows(q), cols] = row_sum(q, q, cols).astype(BF16)

        tile_loop(body)

    def chunk_copy(i, source):
        first, width = CHUNKS[i]
        cols = pl.ds(first, width)
        sems = bulk_s.at[3 + i], bulk_r.at[3 + i]
        return copy_to(across, source.at[rows(0), cols], xr.at[rows(0), cols], *sems)

    def start_chunks(span):
        for i in span:
            late_chunk = CHUNKS[i] in LATE
            start((r == 1) & (core == 0) if late_chunk else r == 1, chunk_copy(i, grad))
            if late_chunk:
                start(r == 0, chunk_copy(i, side))

    arrived(xr.at[rows(3)], bulk_r.at[0])
    push(0)
    far_outer(3, 6, 4)
    block_row(3)
    start(None, bulk(2, 1))
    for h in range(2):

        @pl.when(far_owner)
        def _():
            arrived(far_dst(h), far_r.at[h])

        for n, device in enumerate((mate, next_chip, diagonal)):
            start(far_owner, copy_to(device, far_dst(h), far_dst(h), far_s.at[2 + 3 * h + n], far_r.at[h]))
    push(1)
    add_and_cross(0)
    add_and_cross(1)

    arrived(xr.at[rows(2)], bulk_r.at[1])
    finish_far(1)
    early = range(len(EARLY))
    late = range(len(EARLY), len(CHUNKS))
    start_chunks(early)
    far_outer(2, 8, 4)
    block_row(2)
    push(2)
    finish_local()
    add_and_cross(2)

    arrived(xr.at[rows(1)], bulk_r.at[2])
    start_chunks(late)
    finish_far(2)
    far_outer(1, 10, 2)
    block_row(1)
    push(3)
    weights_here(0)

    @pl.when(r == 0)
    def _():
        corner_weight[...] = wr[0, rows(0)]

    def first_row(cols):
        total = row_sum(0, 1, cols)

        @pl.when(r == 1)
        def _():
            db[rows(0), cols] = total.astype(BF16)

        @pl.when(r == 0)
        def _():
            acc[:, cols] = total

    def first_half(lo, hi):
        def step(j, carry):
            first_row(pl.ds(pl.multiple_of(j * TILE, TILE), TILE))
            return carry

        lax.fori_loop(lo, hi, step, 0)

    add_and_cross(3)
    first_half(0, num_cols // TILE)
    finish_far(3)

    corner[0] = jnp.zeros((BLK, BLK), F32)

    def nt_dot(left, right):
        return lax.dot_general(left, right, (((1,), (1,)), ((), ())), preferred_element_type=F32)

    def corner_in_row(row):
        start((r == row) & (core == 1), copy_to(mate, corner.at[0], corner.at[1], corner_s.at[0], corner_r.at[0]))
        owner = (r == row) & (core == 0)

        @pl.when(owner)
        def _():
            arrived(corner.at[1], corner_r.at[0])
            corner[0] += corner[1]

        start(owner & (x == 1), copy_to(next_chip, corner.at[0], corner.at[2], corner_s.at[1], corner_r.at[1]))

        @pl.when(owner & (x == 0))
        def _():
            arrived(corner.at[2], corner_r.at[1])

        return owner & (x == 0)

    for i, (first, width) in enumerate(CHUNKS):
        early_chunk = (first, width) in EARLY
        here = (r == 0) if early_chunk else (r == 1) | (core == 0)

        @pl.when(here)
        def _():
            arrived(xr.at[rows(0), pl.ds(first, width)], bulk_r.at[3 + i])

            def step(j, carry):
                cols = pl.ds(pl.multiple_of(first + j * TILE, TILE), TILE)

                @pl.when(r == 0)
                def _():
                    term = lax.dot_general(wr[0, rows(0)], xr[rows(0), cols], (((0,), (0,)), ((), ())), preferred_element_type=F32)
                    db[rows(0), cols] = (acc[:, cols] + term).astype(BF16)
                    if early_chunk:
                        corner[0] += nt_dot(xr[rows(0), cols], bl[rows(0), cols])

                if not early_chunk:

                    @pl.when(r == 1)
                    def _():
                        corner[0] += nt_dot(xl[rows(0), cols], xr[rows(0), cols])

                return carry

            lax.fori_loop(0, width // TILE, step, 0)

        if i == len(EARLY) - 1:
            first_device = corner_in_row(0)

            @pl.when(first_device)
            def _():
                corner[0] += corner[2]

            start(first_device, copy_to(across, corner.at[0], corner.at[3], corner_s.at[2], corner_r.at[2]))

    last_device = corner_in_row(1)

    @pl.when(last_device)
    def _():
        arrived(corner.at[3], corner_r.at[2])
        dl[rows(0), rows(0)] = (corner[0] + corner[2] + corner[3]).astype(BF16)

    for i, (p, h) in enumerate(FAR_SLOTS):
        pl.when(other & (x + 2 * h <= p + r - 1))(lambda: arrived(dl.at[rows(p), rows(h)], back_r.at[i]))
    for when, copy in sent:
        if when is None:
            copy.wait_send()
        else:
            pl.when(when)(copy.wait_send)


def per_device(lower, side, grad):
    num_rows, num_cols = grad.shape
    dma = pltpu.SemaphoreType.DMA
    num_bulk = 3 + len(CHUNKS)
    db, dl, acc, weight = pl.pallas_call(
        kernel,
        in_specs=[pl.BlockSpec(memory_space=pl.ANY)] * 3,
        out_specs=[pl.BlockSpec(memory_space=pltpu.VMEM)] * 4,
        out_shape=[pltpu.VMEM(grad.shape, BF16), pltpu.VMEM(lower.shape, BF16), pltpu.VMEM((BLK, num_cols), F32), pltpu.VMEM((BLK, BLK), BF16)],
        scratch_shapes=[
            pltpu.VMEM((num_rows, num_cols), BF16),
            pltpu.VMEM((num_rows, num_cols), BF16),
            pltpu.VMEM((num_rows, num_cols), BF16),
            pltpu.VMEM((4, 4 * BLK, BLK), BF16),
            pltpu.VMEM((4, 4 * BLK, BLK), BF16),
            pltpu.VMEM((2, BLK + SHIFT, BLK), BF16),
            pltpu.VMEM((NUM_SLOTS, 2, BLK, BLK), F32),
            pltpu.VMEM((NUM_SLOTS, 2, BLK, BLK), F32),
            pltpu.VMEM((NUM_SLOTS, BLK, BLK), F32),
            pltpu.VMEM((len(FAR_SLOTS), BLK, BLK), BF16),
            pltpu.VMEM((4, BLK, BLK), F32),
            dma((num_bulk,)), dma((num_bulk,)), dma((8,)), dma((6,)), dma((4,)), dma((8,)), dma((4,)), dma((8,)), dma((2,)), dma((2,)), dma((2,)),
            dma((4,)), dma((4,)), dma((4,)), dma((4,)), dma((5,)), dma((5,)), dma((3,)), dma((3,)),
        ],
        compiler_params=pltpu.CompilerParams(collective_id=0, has_side_effects=True, vmem_limit_bytes=49 * 1024 * 1024),
    )(lower, side, grad)
    in_vmem = pl.BlockSpec(memory_space=pltpu.VMEM)
    anywhere = pl.BlockSpec(memory_space=pl.ANY)

    def keep(value):
        return pltpu.with_memory_space_constraint(value, pltpu.VMEM)

    in_hbm = pl.BlockSpec(memory_space=pltpu.HBM)

    def stay(value):
        return pltpu.with_memory_space_constraint(value, pltpu.HBM)

    db, dl = pl.pallas_call(
        put_kernel,
        in_specs=[in_vmem] * 2,
        out_specs=[anywhere] * 2,
        out_shape=[jax.ShapeDtypeStruct(grad.shape, BF16), jax.ShapeDtypeStruct(lower.shape, BF16)],
        scratch_shapes=[dma((5,))],
        compiler_params=pltpu.CompilerParams(vmem_limit_bytes=1024 * 1024),
    )(keep(db), keep(dl))
    width = sum(w for _, w in LATE)
    tail = pl.pallas_call(
        tail_kernel,
        in_specs=[in_hbm, in_vmem, in_vmem, in_hbm],
        out_specs=in_vmem,
        out_shape=pltpu.VMEM((BLK, width), BF16),
        scratch_shapes=[pltpu.VMEM((BLK, width), BF16), dma((len(LATE),)), dma((len(LATE),))],
        compiler_params=pltpu.CompilerParams(collective_id=1, has_side_effects=True, vmem_limit_bytes=4 * 1024 * 1024),
    )(stay(grad), keep(acc), keep(weight), stay(dl))
    db = pl.pallas_call(
        put_tail_kernel,
        in_specs=[anywhere, in_vmem],
        out_specs=anywhere,
        out_shape=jax.ShapeDtypeStruct(grad.shape, BF16),
        input_output_aliases={0: 0},
        scratch_shapes=[dma],
        compiler_params=pltpu.CompilerParams(vmem_limit_bytes=1024 * 1024),
    )(db, keep(tail))
    return db, dl


def put_kernel(db_in, dl_in, db_out, dl_out, sems):
    copies = [pltpu.make_async_copy(dl_in, dl_out, sems.at[0])]
    copies += [pltpu.make_async_copy(db_in.at[rows(i)], db_out.at[rows(i)], sems.at[1 + i]) for i in range(4)]
    for copy in copies:
        copy.start()
    for copy in copies:
        copy.wait()


def tail_kernel(grad, acc, weight, dl, tail, arriving, send_sem, recv_sem):
    del dl
    r = lax.axis_index("row")
    core = lax.axis_index("col") % 2
    sender = (r == 1) & (core == 1)
    receiver = (r == 0) & (core == 1)
    barrier = pltpu.get_barrier_semaphore()
    pl.when(receiver)(lambda: pl.semaphore_signal(barrier, inc=1, device_id={"row": 1 - r}, device_id_type=MESH))
    pl.when(sender)(lambda: pl.semaphore_wait(barrier, 1))
    base = LATE[0][0]
    copies = []
    for i, (first, width) in enumerate(LATE):
        copies.append(pltpu.make_async_remote_copy(
            src_ref=grad.at[rows(0), pl.ds(first, width)], dst_ref=arriving.at[:, pl.ds(first - base, width)],
            send_sem=send_sem.at[i], recv_sem=recv_sem.at[i], device_id={"row": 1 - r}, device_id_type=MESH))
        pl.when(sender)(copies[i].start)
    for i, (first, width) in enumerate(LATE):

        @pl.when(receiver)
        def _():
            copies[i].wait_recv()
            for n in range(width // TILE):
                at = first - base + n * TILE
                term = lax.dot_general(weight[...], arriving[:, pl.ds(at, TILE)], (((0,), (0,)), ((), ())), preferred_element_type=F32)
                tail[:, pl.ds(at, TILE)] = (acc[:, pl.ds(base + at, TILE)] + term).astype(BF16)

        pl.when(sender)(copies[i].wait_send)


def put_tail_kernel(db_in, tail, db_out, sem):
    del db_in

    @pl.when((lax.axis_index("row") == 0) & (lax.axis_index("col") % 2 == 1))
    def _():
        copy = pltpu.make_async_copy(tail, db_out.at[rows(0), pl.ds(LATE[0][0], tail.shape[1])], sem)
        copy.start()
        copy.wait()


def solution(mesh):
    spec = P(("batch", "row"), "col")
    return jax.shard_map(per_device, mesh=mesh, in_specs=(spec, spec, spec), out_specs=(spec, spec), check_vma=False)
```

```python
import jax
import jax.numpy as jnp
from jax import lax
from jax.experimental import pallas as pl
from jax.experimental.pallas import tpu as pltpu
from jax.sharding import PartitionSpec as P

BLK = 256
F32 = jnp.float32
BF16 = jnp.bfloat16
MESH = pl.DeviceIdType.MESH
TILE = 256
SHIFT = 64
EARLY = ((0, 2304),)
LATE = ((2304, 1536), (3840, 256),)
CHUNKS = EARLY + LATE
LOCAL_SLOTS = ((0, 0), (1, 0), (2, 0), (3, 0), (2, 1), (3, 1))
FAR_SLOTS = ((3, 0), (3, 1), (2, 0), (2, 1), (1, 0))
NUM_LOCAL = len(LOCAL_SLOTS)
NUM_SLOTS = NUM_LOCAL + len(FAR_SLOTS)
GROUPS = ((0, 6), (6, 8), (8, 10), (10, 11))


def rows(p, n=1):
    return pl.ds(p * BLK, n * BLK)


def kernel(lower, side, grad, db, dl, acc, corner_weight, xr, xl, bl, wl, wr, relay, part, peer, cross, done, corner,
           bulk_s, bulk_r, load_s, wl_s, wl_r, near_s, near_r, far_s, far_r, relay_s, relay_r, push_s, push_r, cross_s, cross_r, back_s, back_r, corner_s, corner_r):
    r = lax.axis_index("row")
    c = lax.axis_index("col")
    x = c // 2
    core = c % 2
    own = core == r
    other = core != r
    across = {"row": 1 - r}
    mate = {"col": 2 * x + 1 - core}
    next_chip = {"col": 2 * (1 - x) + core}
    diagonal = {"col": 2 * (1 - x) + 1 - core}
    num_cols = grad.shape[1]
    sent = []

    def copy_to(device, src, dst, send_sem, recv_sem):
        return pltpu.make_async_remote_copy(src_ref=src, dst_ref=dst, send_sem=send_sem, recv_sem=recv_sem, device_id=device, device_id_type=MESH)

    def start(when, copy):
        sent.append((when, copy))
        if when is None:
            copy.start()
        else:
            pl.when(when)(copy.start)

    def arrived(ref, sem):
        pltpu.make_async_copy(ref, ref, sem).wait()

    barrier = pltpu.get_barrier_semaphore()

    def greet(when, *devices):
        @pl.when(when)
        def _():
            for device in devices:
                pl.semaphore_signal(barrier, inc=1, device_id=device, device_id_type=MESH)

    first_core = core == 1
    second_core = core == 0
    greet(first_core, across)
    greet(second_core, across, next_chip)
    pl.when(first_core)(lambda: pl.semaphore_wait(barrier, 1))

    def low_rows(short):
        return pl.ds(3 * BLK + SHIFT, BLK - SHIFT) if short else rows(3)

    def near_src(h, short):
        return lower.at[rows(1, 3), pl.ds(0, BLK)] if h == 0 else lower.at[low_rows(short), pl.ds(BLK, BLK)]

    def near_dst(q, h, short=False):
        return wr.at[q, rows(1, 3)] if h == 0 else wr.at[q, low_rows(short)]

    far_rows = (rows(0), pl.ds(2 * BLK, BLK + SHIFT))
    far_src = tuple(lower.at[far_rows[h], pl.ds(h * BLK, BLK)] for h in range(2))
    far_via = (relay.at[0, pl.ds(0, BLK)], relay.at[1])

    def far_dst(h):
        return wr.at[2 * h, far_rows[h]]

    far_sender = other & (r == 1) & (x == 0)
    near_kinds = ((0, False, other, r >= 0), (1, False, other & jnp.logical_not(far_sender), (r == 1) | (x == 1)), (1, True, far_sender, (r == 0) & (x == 0)))

    def bulk(i, p):
        return copy_to(across, grad.at[rows(p)], xr.at[rows(p)], bulk_s.at[i], bulk_r.at[i])

    def first_copies(when):
        for h, short, sends, _ in near_kinds:
            start(when & sends, copy_to(across, near_src(h, short), near_dst(x + 2 * h, h, short), near_s.at[h], near_r.at[x + 2 * h]))
        start(when, bulk(0, 3))

    first_copies(first_core)
    greet(first_core, mate, diagonal)
    pl.when(second_core)(lambda: pl.semaphore_wait(barrier, 4))
    first_copies(second_core)
    greet(second_core, mate)
    pl.when(first_core)(lambda: pl.semaphore_wait(barrier, 1))

    for h in range(2):
        start(far_sender, copy_to(diagonal, far_src[h], far_via[h], far_s.at[h], relay_r.at[h]))

    loads = [pltpu.make_async_copy(side.at[rows(q)], bl.at[rows(q)], load_s.at[q]) for q in range(4)]
    loads += [pltpu.make_async_copy(grad.at[rows(p)], xl.at[rows(p)], load_s.at[4 + p]) for p in range(4)]
    for load in loads:
        load.start()

    for h in range(2):
        src = lower.at[:, pl.ds(0, BLK)] if h == 0 else lower.at[rows(2, 2), pl.ds(BLK, BLK)]
        q = x + 2 * h
        dst = wl.at[q] if h == 0 else wl.at[q, rows(2, 2)]
        pl.when(own)(pltpu.make_async_copy(src, dst, wl_r.at[q]).start)
        for n, device in enumerate((mate, next_chip, diagonal)):
            start(own, copy_to(device, src, dst, wl_s.at[3 * h + n], wl_r.at[q]))

    @pl.when(r == 1)
    def _():
        wr[2, rows(2)] = jnp.zeros((BLK, BLK), BF16)

    for p in range(4):
        for h in range(2):
            far_zero = (x + 2 * h > p + r - 1) if p else (x >= 0)
            zero = (other & far_zero) | (own & (x + 2 * h > p))

            @pl.when(zero)
            def _():
                dl[rows(p), rows(h)] = jnp.zeros((BLK, BLK), BF16)

    def outer(left, left_row, q):
        total = None
        for k in range(0, num_cols, 1024):
            term = lax.dot_general(left[pl.ds(left_row, BLK), pl.ds(k, 1024)], bl[pl.ds(q * BLK, BLK), pl.ds(k, 1024)], (((1,), (1,)), ((), ())), preferred_element_type=F32)
            total = term if total is None else total + term
        return total

    for load in loads:
        load.wait()

    def local_outer(i, carry):
        slot, parity = i // 2, i % 2
        h = slot // 4
        p = slot - 2 * h
        part[slot, parity] = outer(xl, pl.multiple_of(p * BLK, BLK), 2 * h + parity)
        return carry

    lax.fori_loop(0, 2 * NUM_LOCAL, local_outer, 0)

    for h, short, _, receives in near_kinds:
        q = x + 2 * h
        there = near_dst(q, h, short)
        pl.when(own & receives)(lambda: arrived(there, near_r.at[q]))
        for n, device in enumerate((mate, next_chip, diagonal)):
            start(own & receives, copy_to(device, there, there, near_s.at[2 + 3 * h + n], near_r.at[q]))
    far_owner = other & (r == 0) & (x == 1)
    relay_here = own & (r == 1) & (x == 1)
    for h in range(2):

        @pl.when(relay_here)
        def _():
            arrived(far_via[h], relay_r.at[h])

        start(relay_here, copy_to(across, far_via[h], far_dst(h), relay_s.at[h], far_r.at[h]))
    start(None, bulk(1, 2))

    def push(g):
        lo, hi = GROUPS[g]
        span = pl.ds(lo, hi - lo)
        start(other, copy_to(mate, part.at[span], peer.at[span], push_s.at[g], push_r.at[g]))

    def add_and_cross(g):
        lo, hi = GROUPS[g]
        span = pl.ds(lo, hi - lo)

        @pl.when(own)
        def _():
            arrived(peer.at[span], push_r.at[g])

            def add(slot, carry):
                part[slot] = part[slot] + peer[slot]
                return carry

            lax.fori_loop(lo, hi, add, 0)

        start(own, copy_to(next_chip, part.at[span, 1 - x], cross.at[span], cross_s.at[g], cross_r.at[g]))

    def wait_cross(g):
        lo, hi = GROUPS[g]
        arrived(cross.at[pl.ds(lo, hi - lo)], cross_r.at[g])

    def back_copies(i):
        p, h = FAR_SLOTS[i]
        return copy_to(across, done.at[i], dl.at[rows(p), rows(h)], back_s.at[i], back_r.at[i])

    def finish_far(g):
        lo, hi = GROUPS[g]

        @pl.when(own)
        def _():
            wait_cross(g)
            for slot in range(lo, hi):
                done[slot - NUM_LOCAL] = (part[slot, x] + cross[slot]).astype(BF16)

        for slot in range(lo, hi):
            p, h = FAR_SLOTS[slot - NUM_LOCAL]
            start(own & (x + 2 * h <= p - r), back_copies(slot - NUM_LOCAL))

    def finish_local():
        @pl.when(own)
        def _():
            wait_cross(0)
            below = lax.broadcasted_iota(jnp.int32, (BLK, BLK), 0) >= lax.broadcasted_iota(jnp.int32, (BLK, BLK), 1)
            for slot, (p, h) in enumerate(LOCAL_SLOTS):
                q = x + 2 * h

                @pl.when(q <= p)
                def _():
                    total = part[slot, x] + cross[slot]
                    keep = below | (q < p)
                    dl[rows(p), rows(h)] = jnp.where(keep, total, 0.0).astype(BF16)

    def far_outer(p, lo, num_q):
        def body(q, carry):
            part[lo + q // 2, q % 2] = outer(xr, p * BLK, q)
            return carry

        lax.fori_loop(0, num_q, body, 0)

    def row_sum(q, far_first, cols):
        near = lax.dot_general(wl[q, rows(q, 4 - q)], xl[rows(q, 4 - q), cols], (((0,), (0,)), ((), ())), preferred_element_type=F32)
        far = lax.dot_general(wr[q, rows(far_first, 4 - far_first)], xr[rows(far_first, 4 - far_first), cols], (((0,), (0,)), ((), ())), preferred_element_type=F32)
        return near + far

    def tile_loop(body):
        def step(j, carry):
            body(pl.ds(pl.multiple_of(j * TILE, TILE), TILE))
            return carry

        lax.fori_loop(0, num_cols // TILE, step, 0)

    def weights_here(q):
        h = q // 2
        arrived(wl.at[q] if h == 0 else wl.at[q, rows(2, 2)], wl_r.at[q])
        elsewhere = other | (x + 2 * h != q)
        if q == 2:
            pl.when(elsewhere & (r == 0))(lambda: arrived(near_dst(q, h, True), near_r.at[q]))
            pl.when(elsewhere & (r == 1))(lambda: arrived(near_dst(q, h), near_r.at[q]))
        else:
            pl.when(elsewhere)(lambda: arrived(near_dst(q, h), near_r.at[q]))
        if q % 2 == 0:
            pl.when((r == 0) & jnp.logical_not(far_owner))(lambda: arrived(far_dst(h), far_r.at[h]))

    def block_row(q):
        weights_here(q)

        def body(cols):
            db[rows(q), cols] = row_sum(q, q, cols).astype(BF16)

        tile_loop(body)

    def chunk_copy(i, source):
        first, width = CHUNKS[i]
        cols = pl.ds(first, width)
        sems = bulk_s.at[3 + i], bulk_r.at[3 + i]
        return copy_to(across, source.at[rows(0), cols], xr.at[rows(0), cols], *sems)

    def start_chunks(span):
        for i in span:
            late_chunk = CHUNKS[i] in LATE
            start((r == 1) & (core == 0) if late_chunk else r == 1, chunk_copy(i, grad))
            if late_chunk:
                start(r == 0, chunk_copy(i, side))

    arrived(xr.at[rows(3)], bulk_r.at[0])
    push(0)
    far_outer(3, 6, 4)
    block_row(3)
    start(None, bulk(2, 1))
    for h in range(2):

        @pl.when(far_owner)
        def _():
            arrived(far_dst(h), far_r.at[h])

        for n, device in enumerate((mate, next_chip, diagonal)):
            start(far_owner, copy_to(device, far_dst(h), far_dst(h), far_s.at[2 + 3 * h + n], far_r.at[h]))
    push(1)
    add_and_cross(0)
    add_and_cross(1)

    arrived(xr.at[rows(2)], bulk_r.at[1])
    finish_far(1)
    early = range(len(EARLY))
    late = range(len(EARLY), len(CHUNKS))
    start_chunks(early)
    far_outer(2, 8, 4)
    block_row(2)
    push(2)
    finish_local()
    add_and_cross(2)

    arrived(xr.at[rows(1)], bulk_r.at[2])
    start_chunks(late)
    finish_far(2)
    far_outer(1, 10, 2)
    block_row(1)
    push(3)
    weights_here(0)

    @pl.when(r == 0)
    def _():
        corner_weight[...] = wr[0, rows(0)]

    def first_row(cols):
        total = row_sum(0, 1, cols)

        @pl.when(r == 1)
        def _():
            db[rows(0), cols] = total.astype(BF16)

        @pl.when(r == 0)
        def _():
            acc[:, cols] = total

    def first_half(lo, hi):
        def step(j, carry):
            first_row(pl.ds(pl.multiple_of(j * TILE, TILE), TILE))
            return carry

        lax.fori_loop(lo, hi, step, 0)

    add_and_cross(3)
    first_half(0, num_cols // TILE)
    finish_far(3)

    corner[0] = jnp.zeros((BLK, BLK), F32)

    def nt_dot(left, right):
        return lax.dot_general(left, right, (((1,), (1,)), ((), ())), preferred_element_type=F32)

    def corner_in_row(row):
        start((r == row) & (core == 1), copy_to(mate, corner.at[0], corner.at[1], corner_s.at[0], corner_r.at[0]))
        owner = (r == row) & (core == 0)

        @pl.when(owner)
        def _():
            arrived(corner.at[1], corner_r.at[0])
            corner[0] += corner[1]

        start(owner & (x == 1), copy_to(next_chip, corner.at[0], corner.at[2], corner_s.at[1], corner_r.at[1]))

        @pl.when(owner & (x == 0))
        def _():
            arrived(corner.at[2], corner_r.at[1])

        return owner & (x == 0)

    for i, (first, width) in enumerate(CHUNKS):
        early_chunk = (first, width) in EARLY
        here = (r == 0) if early_chunk else (r == 1) | (core == 0)

        @pl.when(here)
        def _():
            arrived(xr.at[rows(0), pl.ds(first, width)], bulk_r.at[3 + i])

            def step(j, carry):
                cols = pl.ds(pl.multiple_of(first + j * TILE, TILE), TILE)

                @pl.when(r == 0)
                def _():
                    term = lax.dot_general(wr[0, rows(0)], xr[rows(0), cols], (((0,), (0,)), ((), ())), preferred_element_type=F32)
                    db[rows(0), cols] = (acc[:, cols] + term).astype(BF16)
                    if early_chunk:
                        corner[0] += nt_dot(xr[rows(0), cols], bl[rows(0), cols])

                if not early_chunk:

                    @pl.when(r == 1)
                    def _():
                        corner[0] += nt_dot(xl[rows(0), cols], xr[rows(0), cols])

                return carry

            lax.fori_loop(0, width // TILE, step, 0)

        if i == len(EARLY) - 1:
            first_device = corner_in_row(0)

            @pl.when(first_device)
            def _():
                corner[0] += corner[2]

            start(first_device, copy_to(across, corner.at[0], corner.at[3], corner_s.at[2], corner_r.at[2]))

    last_device = corner_in_row(1)

    @pl.when(last_device)
    def _():
        arrived(corner.at[3], corner_r.at[2])
        dl[rows(0), rows(0)] = (corner[0] + corner[2] + corner[3]).astype(BF16)

    for i, (p, h) in enumerate(FAR_SLOTS):
        pl.when(other & (x + 2 * h <= p + r - 1))(lambda: arrived(dl.at[rows(p), rows(h)], back_r.at[i]))
    for when, copy in sent:
        if when is None:
            copy.wait_send()
        else:
            pl.when(when)(copy.wait_send)


def per_device(lower, side, grad):
    num_rows, num_cols = grad.shape
    dma = pltpu.SemaphoreType.DMA
    num_bulk = 3 + len(CHUNKS)
    db, dl, acc, weight = pl.pallas_call(
        kernel,
        in_specs=[pl.BlockSpec(memory_space=pl.ANY)] * 3,
        out_specs=[pl.BlockSpec(memory_space=pltpu.VMEM)] * 4,
        out_shape=[pltpu.VMEM(grad.shape, BF16), pltpu.VMEM(lower.shape, BF16), pltpu.VMEM((BLK, num_cols), F32), pltpu.VMEM((BLK, BLK), BF16)],
        scratch_shapes=[
            pltpu.VMEM((num_rows, num_cols), BF16),
            pltpu.VMEM((num_rows, num_cols), BF16),
            pltpu.VMEM((num_rows, num_cols), BF16),
            pltpu.VMEM((4, 4 * BLK, BLK), BF16),
            pltpu.VMEM((4, 4 * BLK, BLK), BF16),
            pltpu.VMEM((2, BLK + SHIFT, BLK), BF16),
            pltpu.VMEM((NUM_SLOTS, 2, BLK, BLK), F32),
            pltpu.VMEM((NUM_SLOTS, 2, BLK, BLK), F32),
            pltpu.VMEM((NUM_SLOTS, BLK, BLK), F32),
            pltpu.VMEM((len(FAR_SLOTS), BLK, BLK), BF16),
            pltpu.VMEM((4, BLK, BLK), F32),
            dma((num_bulk,)), dma((num_bulk,)), dma((8,)), dma((6,)), dma((4,)), dma((8,)), dma((4,)), dma((8,)), dma((2,)), dma((2,)), dma((2,)),
            dma((4,)), dma((4,)), dma((4,)), dma((4,)), dma((5,)), dma((5,)), dma((3,)), dma((3,)),
        ],
        compiler_params=pltpu.CompilerParams(collective_id=0, has_side_effects=True, vmem_limit_bytes=49 * 1024 * 1024),
    )(lower, side, grad)
    in_vmem = pl.BlockSpec(memory_space=pltpu.VMEM)
    anywhere = pl.BlockSpec(memory_space=pl.ANY)

    def keep(value):
        return pltpu.with_memory_space_constraint(value, pltpu.VMEM)

    in_hbm = pl.BlockSpec(memory_space=pltpu.HBM)

    def stay(value):
        return pltpu.with_memory_space_constraint(value, pltpu.HBM)

    db, dl = pl.pallas_call(
        put_kernel,
        in_specs=[in_vmem] * 2,
        out_specs=[anywhere] * 2,
        out_shape=[jax.ShapeDtypeStruct(grad.shape, BF16), jax.ShapeDtypeStruct(lower.shape, BF16)],
        scratch_shapes=[dma((5,))],
        compiler_params=pltpu.CompilerParams(vmem_limit_bytes=1024 * 1024),
    )(keep(db), keep(dl))
    width = sum(w for _, w in LATE)
    tail, arrived = pl.pallas_call(
        tail_kernel,
        in_specs=[in_hbm, in_vmem, in_vmem, in_hbm],
        out_specs=[in_vmem] * 2,
        out_shape=[pltpu.VMEM((BLK, width), BF16)] * 2,
        scratch_shapes=[dma((len(LATE),)), dma((len(LATE),))],
        compiler_params=pltpu.CompilerParams(collective_id=1, has_side_effects=True, vmem_limit_bytes=4 * 1024 * 1024),
    )(stay(grad), keep(acc), keep(weight), stay(dl))
    db = pl.pallas_call(
        put_tail_kernel,
        in_specs=[anywhere] + [in_vmem] * 4,
        out_specs=anywhere,
        out_shape=jax.ShapeDtypeStruct(grad.shape, BF16),
        input_output_aliases={0: 0},
        scratch_shapes=[pltpu.VMEM((BLK, LATE[-1][1]), BF16), dma((2,))],
        compiler_params=pltpu.CompilerParams(vmem_limit_bytes=4 * 1024 * 1024),
    )(db, keep(tail), keep(arrived), keep(acc), keep(weight))
    return db, dl


def put_kernel(db_in, dl_in, db_out, dl_out, sems):
    copies = [pltpu.make_async_copy(dl_in, dl_out, sems.at[0])]
    copies += [pltpu.make_async_copy(db_in.at[rows(i)], db_out.at[rows(i)], sems.at[1 + i]) for i in range(4)]
    for copy in copies:
        copy.start()
    for copy in copies:
        copy.wait()


def finished(weight, block, start_value):
    return (start_value + lax.dot_general(weight, block, (((0,), (0,)), ((), ())), preferred_element_type=F32)).astype(BF16)


def tail_kernel(grad, acc, weight, dl, tail, arriving, send_sem, recv_sem):
    del dl
    r = lax.axis_index("row")
    core = lax.axis_index("col") % 2
    sender = (r == 1) & (core == 1)
    receiver = (r == 0) & (core == 1)
    barrier = pltpu.get_barrier_semaphore()
    pl.when(receiver)(lambda: pl.semaphore_signal(barrier, inc=1, device_id={"row": 1 - r}, device_id_type=MESH))
    pl.when(sender)(lambda: pl.semaphore_wait(barrier, 1))
    base = LATE[0][0]
    copies = []
    for i, (first, width) in enumerate(LATE):
        copies.append(pltpu.make_async_remote_copy(
            src_ref=grad.at[rows(0), pl.ds(first, width)], dst_ref=arriving.at[:, pl.ds(first - base, width)],
            send_sem=send_sem.at[i], recv_sem=recv_sem.at[i], device_id={"row": 1 - r}, device_id_type=MESH))
        pl.when(sender)(copies[i].start)
    for i, (first, width) in enumerate(LATE):

        @pl.when(receiver)
        def _():
            copies[i].wait_recv()
            if i < len(LATE) - 1:
                for n in range(width // TILE):
                    at = first - base + n * TILE
                    tail[:, pl.ds(at, TILE)] = finished(weight[...], arriving[:, pl.ds(at, TILE)], acc[:, pl.ds(base + at, TILE)])

        pl.when(sender)(copies[i].wait_send)


def put_tail_kernel(db_in, tail, arrived, acc, weight, db_out, last, sems):
    del db_in
    base = LATE[0][0]
    first, width = LATE[-1]

    @pl.when((lax.axis_index("row") == 0) & (lax.axis_index("col") % 2 == 1))
    def _():
        ready = pltpu.make_async_copy(tail.at[:, pl.ds(0, first - base)], db_out.at[rows(0), pl.ds(base, first - base)], sems.at[0])
        ready.start()
        last[...] = finished(weight[...], arrived[:, pl.ds(first - base, width)], acc[:, pl.ds(first, width)])
        rest = pltpu.make_async_copy(last, db_out.at[rows(0), pl.ds(first, width)], sems.at[1])
        rest.start()
        ready.wait()
        rest.wait()


def solution(mesh):
    spec = P(("batch", "row"), "col")
    return jax.shard_map(per_device, mesh=mesh, in_specs=(spec, spec, spec), out_specs=(spec, spec), check_vma=False)
```
